128 devices in a mesh: dp: 1, sp: 128 (over z, y, x, core).
Axes of the slice: x: 4, y: 4, z: 4, core: 2. Of those that a mesh axis runs over, the one named last changes fastest.
Arguments:
- y_dec: bfloat16 [2048, 768], P(('dp', 'sp'))
- memory: bfloat16 [131072, 768], P(('dp', 'sp'))
- mem_len: int32 [1], P('dp')
- norm_gain: bfloat16 [2, 768], replicated
- self_wq: bfloat16 [2, 768, 768], replicated
- self_wk: bfloat16 [2, 768, 768], replicated
- self_wv: bfloat16 [2, 768, 768], replicated
- self_wo: bfloat16 [2, 768, 768], replicated
- cross_wq: bfloat16 [2, 768, 768], replicated
- cross_wk: bfloat16 [2, 768, 768], replicated
- cross_wv: bfloat16 [2, 768, 768], replicated
- cross_wo: bfloat16 [2, 768, 768], replicated
- mlp_gate: bfloat16 [2, 768, 2048], replicated
- mlp_up: bfloat16 [2, 768, 2048], replicated
- mlp_down: bfloat16 [2, 2048, 768], replicated
Outputs:
- output: bfloat16 [2048, 768], P(('dp', 'sp'))
All inputs are finite; a program needn't handle non-finite values.
Results may differ from the reference program's by a relative error of at most 0.0105201.
Values are sent between devices in bfloat16 or wider.
A program may use at most 1 GiB of HBM per device.

```python
import jax
import jax.numpy as jnp
from jax import lax

D = 768
HEADS = 12
KV_HEADS = 12
HEAD = 64
FF = 2048
LAYERS = 2
GROUP = 128
TQ_DEV = 16
TM_DEV = 1024

TQ = GROUP * TQ_DEV
TM = GROUP * TM_DEV
DKV = KV_HEADS * HEAD
QGROUP = HEADS // KV_HEADS
SCORE_SCALE = HEAD ** -0.5
NORM_EPS = 1e-6
NEG_BIG = -1e30


def scaled_normal(rng_key, arr_shape, fan_in):
    drawn = jax.random.normal(rng_key, arr_shape, jnp.float32) * fan_in ** -0.5
    return drawn.astype(jnp.bfloat16)


def setup_inputs(seed: int = 0, part: int = 0) -> dict:
    root_key = jax.random.key(seed)
    data_root, weight_root = jax.random.split(root_key)
    data_key = jax.random.fold_in(data_root, part)
    data_keys = jax.random.split(data_key, 6)
    dec_noise = jax.random.normal(data_keys[0], (GROUP, TQ_DEV, D), jnp.float32)
    dec_topic = jax.random.normal(data_keys[1], (GROUP, 1, D), jnp.float32)
    dec_amp = jax.random.uniform(data_keys[2], (GROUP, 1, 1), jnp.float32, 0.5, 1.5)
    y_dec = (dec_noise + dec_amp * dec_topic).reshape(TQ, D).astype(jnp.bfloat16)
    mem_noise = jax.random.normal(data_keys[3], (GROUP, TM_DEV, D), jnp.float32)
    mem_topic = jax.random.normal(data_keys[4], (GROUP, 1, D), jnp.float32)
    mem_amp = jax.random.uniform(data_keys[5], (GROUP, 1, 1), jnp.float32, 0.5, 2.0)
    memory = (mem_noise + mem_amp * mem_topic).reshape(TM, D).astype(jnp.bfloat16)
    len_key = jax.random.fold_in(data_key, 11)
    mem_len = jax.random.randint(len_key, (1,), TM // 4, (3 * TM) // 4, jnp.int32)
    weight_keys = jax.random.split(weight_root, 12)
    norm_gain = (1.0 + 0.25 * jax.random.normal(weight_keys[0], (LAYERS, D), jnp.float32)).astype(jnp.bfloat16)
    return {
        "y_dec": y_dec,
        "memory": memory,
        "mem_len": mem_len,
        "norm_gain": norm_gain,
        "self_wq": scaled_normal(weight_keys[1], (LAYERS, D, D), D),
        "self_wk": scaled_normal(weight_keys[2], (LAYERS, D, D), D),
        "self_wv": scaled_normal(weight_keys[3], (LAYERS, D, D), D),
        "self_wo": scaled_normal(weight_keys[4], (LAYERS, D, D), D),
        "cross_wq": scaled_normal(weight_keys[5], (LAYERS, D, D), D),
        "cross_wk": scaled_normal(weight_keys[6], (LAYERS, D, DKV), D),
        "cross_wv": scaled_normal(weight_keys[7], (LAYERS, D, DKV), D),
        "cross_wo": scaled_normal(weight_keys[8], (LAYERS, D, D), D),
        "mlp_gate": scaled_normal(weight_keys[9], (LAYERS, D, FF), D),
        "mlp_up": scaled_normal(weight_keys[10], (LAYERS, D, FF), D),
        "mlp_down": scaled_normal(weight_keys[11], (LAYERS, FF, D), FF),
    }


def matmul(left_mat, right_mat):
    return jnp.dot(left_mat, right_mat, preferred_element_type=jnp.float32)


def rms_norm(hidden, gain_vec):
    wide_vals = hidden.astype(jnp.float32)
    inv_rms = lax.rsqrt(jnp.mean(wide_vals * wide_vals, axis=-1, keepdims=True) + NORM_EPS)
    return (wide_vals * inv_rms * gain_vec.astype(jnp.float32)).astype(jnp.bfloat16)


def reference(y_dec, memory, mem_len, norm_gain, self_wq, self_wk, self_wv, self_wo, cross_wq, cross_wk, cross_wv, cross_wo, mlp_gate, mlp_up, mlp_down):
    key_pos = jnp.arange(TQ)
    mem_valid = jnp.arange(TM) < mem_len[0]
    block_ids = jnp.arange(GROUP)

    def layer_step(hidden, layer_weights):
        gain_vec, self_q, self_k, self_v, self_o, cross_q, cross_k, cross_v, cross_o, gate_w, up_w, down_w = layer_weights
        normed = rms_norm(hidden, gain_vec)
        query_self = matmul(normed, self_q).astype(jnp.bfloat16).reshape(GROUP, TQ_DEV, HEADS, HEAD)
        key_self = matmul(normed, self_k).astype(jnp.bfloat16).reshape(TQ, HEADS, HEAD).astype(jnp.float32)
        value_self = matmul(normed, self_v).astype(jnp.bfloat16).reshape(TQ, HEADS, HEAD).astype(jnp.float32)

        def self_block(block_in):
            query_blk, block_id = block_in
            scores = jnp.einsum("qhd,khd->hqk", query_blk.astype(jnp.float32), key_self) * SCORE_SCALE
            query_pos = block_id * TQ_DEV + jnp.arange(TQ_DEV)
            causal = key_pos[None, :] <= query_pos[:, None]
            scores = jnp.where(causal[None], scores, NEG_BIG)
            self_probs = jax.nn.softmax(scores, axis=-1).astype(jnp.bfloat16)
            return jnp.einsum("hqk,khd->qhd", self_probs.astype(jnp.float32), value_self)

        self_heads = lax.map(self_block, (query_self, block_ids))
        self_part = matmul(self_heads.reshape(TQ, D).astype(jnp.bfloat16), self_o)

        query_cross = matmul(normed, cross_q).astype(jnp.bfloat16).reshape(GROUP, TQ_DEV, KV_HEADS, QGROUP, HEAD)
        key_mem = matmul(memory, cross_k).astype(jnp.bfloat16).reshape(TM, KV_HEADS, HEAD).astype(jnp.float32)
        value_mem = matmul(memory, cross_v).astype(jnp.bfloat16).reshape(TM, KV_HEADS, HEAD).astype(jnp.float32)

        def cross_block(query_blk):
            scores = jnp.einsum("qkgd,mkd->kgqm", query_blk.astype(jnp.float32), key_mem) * SCORE_SCALE
            scores = jnp.where(mem_valid, scores, NEG_BIG)
            cross_probs = jax.nn.softmax(scores, axis=-1).astype(jnp.bfloat16)
            return jnp.einsum("kgqm,mkd->qkgd", cross_probs.astype(jnp.float32), value_mem)

        cross_heads = lax.map(cross_block, query_cross)
        cross_part = matmul(cross_heads.reshape(TQ, D).astype(jnp.bfloat16), cross_o)

        activated = (jax.nn.silu(matmul(normed, gate_w)) * matmul(normed, up_w)).astype(jnp.bfloat16)
        mlp_part = matmul(activated, down_w)
        new_hidden = (hidden.astype(jnp.float32) + self_part + cross_part + mlp_part).astype(jnp.bfloat16)
        return new_hidden, None

    stacked = (norm_gain, self_wq, self_wk, self_wv, self_wo, cross_wq, cross_wk, cross_wv, cross_wo, mlp_gate, mlp_up, mlp_down)
    final_hidden, unused = lax.scan(layer_step, y_dec, stacked)
    return final_hidden
```

```python
import functools
import math

import jax
import jax.numpy as jnp
from jax import lax
from jax.experimental import pallas as pl
from jax.experimental.pallas import tpu as pltpu
from jax.sharding import PartitionSpec as P

HEAD = 64
NORM_EPS = 1e-6
NEG_BIG = -1e30
MESH = pl.DeviceIdType.MESH
EXP_SCALE = HEAD ** -0.5 * math.log2(math.e)
ORDERS = ((0, 1, 2), (1, 2, 0), (2, 0, 1))
VMEM_SPEC = pl.BlockSpec(memory_space=pltpu.VMEM)
ROW_TILE = 512


def matmul(left_mat, right_mat):
    return jnp.dot(left_mat, right_mat, preferred_element_type=jnp.float32)


def rms_norm(hidden, gain_vec):
    wide_vals = hidden.astype(jnp.float32)
    inv_rms = lax.rsqrt(jnp.mean(wide_vals * wide_vals, axis=-1, keepdims=True) + NORM_EPS)
    return (wide_vals * inv_rms * gain_vec.astype(jnp.float32)).astype(jnp.bfloat16)


def coords():
    sp = lax.axis_index("sp")
    return (sp // 32, (sp // 8) % 4, (sp // 2) % 4), sp % 2


def device_of(pos, core):
    return {"sp": ((pos[0] * 4 + pos[1]) * 4 + pos[2]) * 2 + core}


def shifted(pos, axis, dist):
    return tuple((c + dist) % 4 if i == axis else c for i, c in enumerate(pos))


def entry_barrier(pos, core):
    sem = pltpu.get_barrier_semaphore()
    for axis in range(3):
        for dist in (1, 2, 3):
            pl.semaphore_signal(sem, inc=1, device_id=device_of(shifted(pos, axis, dist), core), device_id_type=MESH)
    pl.semaphore_signal(sem, inc=1, device_id=device_of(pos, 1 - core), device_id_type=MESH)
    pl.semaphore_wait(sem, 10)


def swap_kernel(mem_ref, out_ref, local_sem, send_sem, recv_sem):
    pos, core = coords()
    sem = pltpu.get_barrier_semaphore()
    other = device_of(pos, 1 - core)
    pl.semaphore_signal(sem, inc=1, device_id=other, device_id_type=MESH)
    pl.semaphore_wait(sem, 1)
    remote = pltpu.make_async_remote_copy(
        src_ref=mem_ref, dst_ref=out_ref.at[core], send_sem=send_sem, recv_sem=recv_sem,
        device_id=other, device_id_type=MESH)
    remote.start()
    local = pltpu.make_async_copy(mem_ref, out_ref.at[core], local_sem)
    local.start()
    local.wait()
    remote.wait()


def swap_memory(memory):
    rows, width = memory.shape
    return pl.pallas_call(
        swap_kernel,
        out_shape=jax.ShapeDtypeStruct((2, rows, width), memory.dtype),
        in_specs=[VMEM_SPEC],
        out_specs=pl.BlockSpec(memory_space=pl.ANY),
        scratch_shapes=[pltpu.SemaphoreType.DMA] * 3,
        compiler_params=pltpu.CompilerParams(collective_id=0, has_side_effects=True),
        name="swap_memory",
    )(memory)


def gather_slice(ref, part, order, free, pos, core):
    idx = [part]
    for axis in range(3):
        idx.append(slice(None) if axis in free else pos[axis])
    return ref.at[tuple(idx) + (core,)]


def gather_kernel(x_ref, out_ref, local_sem, send_sem, recv_sem, sib_send, sib_recv):
    pos, core = coords()
    entry_barrier(pos, core)
    sibling = device_of(pos, 1 - core)

    def phase_copy(part, phase, dist):
        order = ORDERS[part]
        if phase == 0:
            src = x_ref.at[part]
        else:
            src = gather_slice(out_ref, part, order, order[:phase], pos, core)
        dst = gather_slice(out_ref, part, order, order[:phase], pos, core)
        return pltpu.make_async_remote_copy(
            src_ref=src, dst_ref=dst, send_sem=send_sem.at[part, phase, dist - 1],
            recv_sem=recv_sem.at[part, phase, dist - 1],
            device_id=device_of(shifted(pos, order[phase], dist), core), device_id_type=MESH)

    def sibling_copy(part, dist):
        order = ORDERS[part]
        at = shifted(pos, order[2], 4 - dist)
        ref = gather_slice(out_ref, part, order, order[:2], at, core)
        return pltpu.make_async_remote_copy(
            src_ref=ref, dst_ref=ref, send_sem=sib_send.at[part, dist], recv_sem=sib_recv.at[part, dist],
            device_id=sibling, device_id_type=MESH)

    local = [pltpu.make_async_copy(x_ref.at[p], gather_slice(out_ref, p, ORDERS[p], (), pos, core), local_sem.at[p])
             for p in range(3)]
    copies = {}
    for phase in range(3):
        for part in range(3):
            if phase == 1:
                local[part].wait()
            if phase > 0:
                for dist in (1, 2, 3):
                    copies[part, phase - 1, dist].wait_recv()
            for dist in (2, 1, 3):
                copies[part, phase, dist] = phase_copy(part, phase, dist)
                copies[part, phase, dist].start()
            if phase == 0:
                local[part].start()
            if phase == 2:
                copies[part, 3, 0] = sibling_copy(part, 0)
                copies[part, 3, 0].start()
    for dist in (1, 3, 2):
        for part in range(3):
            copies[part, 2, dist].wait_recv()
            copies[part, 3, dist] = sibling_copy(part, dist)
            copies[part, 3, dist].start()
    for part in range(3):
        for dist in range(4):
            copies[part, 3, dist].wait_recv()
    for copy in copies.values():
        copy.wait_send()


def gather_rows(normed):
    rows, width = normed.shape
    parts = normed.reshape(rows, 3, width // 3).transpose(1, 0, 2)
    gathered = pl.pallas_call(
        gather_kernel,
        out_shape=jax.ShapeDtypeStruct((3, 4, 4, 4, 2, rows, width // 3), normed.dtype),
        in_specs=[VMEM_SPEC],
        out_specs=VMEM_SPEC,
        scratch_shapes=[pltpu.SemaphoreType.DMA((3,)), pltpu.SemaphoreType.DMA((3, 3, 3)),
                        pltpu.SemaphoreType.DMA((3, 3, 3)), pltpu.SemaphoreType.DMA((3, 4)),
                        pltpu.SemaphoreType.DMA((3, 4))],
        compiler_params=pltpu.CompilerParams(collective_id=1, has_side_effects=True),
        name="gather_rows",
    )(parts)
    return gathered.reshape(3, 4, 4, 4, 2 * rows, width // 3)


def self_kernel(info_ref, h_ref, wq_ref, wk_ref, wv_ref, cq_ref, att_ref, qt_ref, k_ref, v_ref):
    core_heads = wq_ref.shape[1]
    chip = info_ref[0]
    hz, hy, hx = chip // 16, (chip // 4) % 4, chip % 4

    def rows_cat(z, y, x):
        return jnp.concatenate([h_ref[p, z, y, x] for p in range(3)], axis=1)

    def key_tile(zy, carry):
        z, y = zy // 4, zy % 4
        rows = jnp.concatenate([rows_cat(z, y, x) for x in range(4)], axis=0)
        at = pl.ds(pl.multiple_of(zy * 128, 128), 128)
        k_ref[at, :] = matmul(rows, wk_ref[...]).astype(jnp.bfloat16)
        v_ref[at, :] = matmul(rows, wv_ref[...]).astype(jnp.bfloat16)
        return carry

    lax.fori_loop(0, 16, key_tile, 0)

    for part in range(3):
        cols = slice(part * 128, part * 128 + 128)

        def query_tile(ab, carry, part=part, cols=cols):
            order = ORDERS[part]
            blocks = []
            for c in range(4):
                at = [None] * 3
                at[order[0]], at[order[1]], at[order[2]] = ab // 4, ab % 4, c
                blocks.append(rows_cat(*at))
            rows = jnp.concatenate(blocks, axis=0)
            q = matmul(rows, cq_ref[:, cols])
            qt_ref[part, ab] = jnp.transpose(q).astype(jnp.bfloat16)
            return carry

        lax.fori_loop(0, 16, query_tile, 0)

    rows = rows_cat(hz, hy, hx)
    query = matmul(rows, wq_ref[...]).astype(jnp.bfloat16)
    n_query = rows.shape[0]
    n_keys = k_ref.shape[0]
    low = lax.broadcasted_iota(jnp.int32, (n_query, 128), 1) < HEAD
    key_pos = lax.broadcasted_iota(jnp.int32, (n_query, n_keys), 1)
    query_pos = chip * n_query + lax.broadcasted_iota(jnp.int32, (n_query, n_keys), 0)
    causal = key_pos <= query_pos
    for part in range(core_heads // 128):
        cols = slice(part * 128, part * 128 + 128)
        q_pair = query[:, cols]
        outs = []
        for head in range(2):
            mask = low if head == 0 else jnp.logical_not(low)
            q_one = jnp.where(mask, q_pair, jnp.zeros_like(q_pair))
            s = lax.dot_general(q_one, k_ref[:, cols], (((1,), (1,)), ((), ())), preferred_element_type=jnp.float32)
            s = jnp.where(causal, s, NEG_BIG)
            top = jnp.max(s, axis=1, keepdims=True)
            w = jnp.exp2((s - top) * EXP_SCALE)
            total = jnp.sum(w, axis=1, keepdims=True)
            o = matmul(w.astype(jnp.bfloat16), v_ref[:, cols])
            outs.append(o / total)
        att_ref[:, cols] = jnp.where(low, outs[0], outs[1]).astype(jnp.bfloat16)


def self_attention(info, gathered, layer, wq, wk, wv, cq):
    width = wq.shape[1]
    half = width // 2
    n_rows = 64 * gathered.shape[4]
    w_spec = pl.BlockSpec((None, width, half), lambda i, info: (layer, 0, info[1]))
    return pl.pallas_call(
        self_kernel,
        grid_spec=pltpu.PrefetchScalarGridSpec(
            num_scalar_prefetch=1,
            grid=(1,),
            in_specs=[pl.BlockSpec(gathered.shape, lambda i, info: (0,) * 6)] + [w_spec] * 4,
            out_specs=[pl.BlockSpec((n_rows // 64, half), lambda i, info: (0, 0)),
                       pl.BlockSpec((3, 16, 128, 128), lambda i, info: (0, 0, 0, 0))],
            scratch_shapes=[pltpu.VMEM((n_rows, half), jnp.bfloat16)] * 2,
        ),
        out_shape=[jax.ShapeDtypeStruct((n_rows // 64, half), jnp.bfloat16),
                   jax.ShapeDtypeStruct((3, 16, 128, 128), jnp.bfloat16)],
        compiler_params=pltpu.CompilerParams(vmem_limit_bytes=48 * 1024 * 1024),
        name="self_attention",
    )(info, gathered, wq, wk, wv, cq)


def kv_kernel(info_ref, m_ref, wk_ref, wv_ref, k_ref, vt_ref):
    @pl.when(pl.program_id(1) < info_ref[3])
    def _():
        rows = m_ref[...]
        k_ref[...] = matmul(rows, wk_ref[...]).astype(jnp.bfloat16)
        vt_ref[...] = jnp.transpose(matmul(rows, wv_ref[...])).astype(jnp.bfloat16)


def memory_kv(info, chip_memory, wk, wv):
    n_rows, width = chip_memory.shape
    half = width // 2
    layers = wk.shape[0]
    w_spec = pl.BlockSpec((None, width, half), lambda l, t, info: (l, 0, info[1]))
    return pl.pallas_call(
        kv_kernel,
        grid_spec=pltpu.PrefetchScalarGridSpec(
            num_scalar_prefetch=1,
            grid=(layers, n_rows // ROW_TILE),
            in_specs=[pl.BlockSpec((ROW_TILE, width), lambda l, t, info: (t, 0)), w_spec, w_spec],
            out_specs=[pl.BlockSpec((None, ROW_TILE, half), lambda l, t, info: (l, t, 0)),
                       pl.BlockSpec((None, half, ROW_TILE), lambda l, t, info: (l, 0, t))],
        ),
        out_shape=[jax.ShapeDtypeStruct((layers, n_rows, half), jnp.bfloat16),
                   jax.ShapeDtypeStruct((layers, half, n_rows), jnp.bfloat16)],
        compiler_params=pltpu.CompilerParams(vmem_limit_bytes=48 * 1024 * 1024),
        name="memory_kv",
    )(info, chip_memory, wk, wv)


def cross_kernel(info_ref, qt_ref, k_ref, vt_ref, out_ref, acc_ref):
    n_valid = info_ref[2]
    n_tiles = info_ref[3]
    n_q = 512
    qt = jnp.concatenate([qt_ref[i] for i in range(4)], axis=1)
    low = lax.broadcasted_iota(jnp.int32, (128, n_q), 0) < HEAD
    zero = jnp.zeros_like(qt)
    ones = jnp.where(lax.broadcasted_iota(jnp.int32, (128, n_q), 0) == 0, 1.0, 0.0).astype(jnp.bfloat16)
    q_heads = (jnp.concatenate([jnp.where(low, qt, zero), ones], axis=0),
               jnp.concatenate([jnp.where(low, zero, qt), ones], axis=0))
    acc_ref[...] = jnp.zeros_like(acc_ref)

    def row_tile(t, carry):
        at = pl.ds(pl.multiple_of(t * ROW_TILE, ROW_TILE), ROW_TILE)
        row = t * ROW_TILE + lax.broadcasted_iota(jnp.int32, (ROW_TILE, 128), 0)
        bias = jnp.where(row < n_valid, 0.0, NEG_BIG).astype(jnp.bfloat16)
        keys = jnp.concatenate([k_ref[at, :], bias], axis=1)
        new = []
        for head in range(2):
            top, total = carry[2 * head], carry[2 * head + 1]
            s = matmul(keys, q_heads[head])
            new_top = jnp.maximum(top, jnp.max(s, axis=0, keepdims=True) * EXP_SCALE)
            w = jnp.exp2(s * EXP_SCALE - new_top)
            fix = jnp.exp2(top - new_top)
            new += [new_top, total * fix + jnp.sum(w, axis=0, keepdims=True)]
            vals = slice(head * HEAD, head * HEAD + HEAD)
            acc_ref[vals, :] = acc_ref[vals, :] * fix + matmul(vt_ref[vals, at], w.astype(jnp.bfloat16))
        return tuple(new)

    init = (jnp.full((1, n_q), NEG_BIG, jnp.float32), jnp.zeros((1, n_q), jnp.float32)) * 2
    t0, l0, t1, l1 = lax.fori_loop(0, n_tiles, row_tile, init)
    out_ref[0:128, :] = acc_ref[...]
    out_ref[128:136, :] = jnp.concatenate([t0, t1, l0, l1, t0, t1, l0, l1], axis=0)


def cross_attention(info, layer, qt, keys, values):
    n_rows = keys.shape[1]
    return pl.pallas_call(
        cross_kernel,
        grid_spec=pltpu.PrefetchScalarGridSpec(
            num_scalar_prefetch=1,
            grid=(3, 4),
            in_specs=[pl.BlockSpec((None, 4, 128, 128), lambda p, j, info: (p, j, 0, 0)),
                      pl.BlockSpec((None, n_rows, 128), lambda p, j, info: (layer, 0, p)),
                      pl.BlockSpec((None, 128, n_rows), lambda p, j, info: (layer, p, 0))],
            out_specs=pl.BlockSpec((None, None, 136, 512), lambda p, j, info: (p, j, 0, 0)),
            scratch_shapes=[pltpu.VMEM((128, 512), jnp.float32)],
        ),
        out_shape=jax.ShapeDtypeStruct((3, 4, 136, 512), jnp.float32),
        compiler_params=pltpu.CompilerParams(vmem_limit_bytes=48 * 1024 * 1024),
        name="cross_attention",
    )(info, qt, keys, values)


def merge(pieces):
    tops = [p[128:130] for p in pieces]
    sums = [p[130:132] for p in pieces]
    top = functools.reduce(jnp.maximum, tops)
    fixes = [jnp.exp2(t - top) for t in tops]
    total = functools.reduce(jnp.add, [f * s for f, s in zip(fixes, sums)])
    outs = []
    for head in range(2):
        rows = slice(head * HEAD, head * HEAD + HEAD)
        outs.append(functools.reduce(jnp.add, [p[rows] * f[head:head + 1] for p, f in zip(pieces, fixes)]))
    return outs, top, total


def merge_kernel(part_ref, att_ref, out_ref, recv1, acc1, recv2, acc2, recv3, turned, mine,
                 send_sem, recv_sem, sib_send, sib_recv):
    pos, core = coords()
    entry_barrier(pos, core)

    def copy(part, phase, dist):
        axis = ORDERS[part][phase]
        peer = shifted(pos, axis, dist)
        src, dst = ((part_ref.at[part, peer[axis]], recv1.at[part, dist - 1]),
                    (acc1.at[part, peer[axis]], recv2.at[part, dist - 1]),
                    (acc2.at[part], recv3.at[part, dist - 1]))[phase]
        return pltpu.make_async_remote_copy(
            src_ref=src, dst_ref=dst, send_sem=send_sem.at[part, phase, dist - 1],
            recv_sem=recv_sem.at[part, phase, dist - 1], device_id=device_of(peer, core), device_id_type=MESH)

    copies = {}

    def start(part, phase):
        for dist in (2, 1, 3):
            copies[part, phase, dist] = copy(part, phase, dist)
            copies[part, phase, dist].start()

    for part in range(3):
        start(part, 0)
    for part in range(3):
        for dist in (1, 2, 3):
            copies[part, 0, dist].wait_recv()
        own = pos[ORDERS[part][0]]
        for b in range(4):
            lanes = slice(b * 128, b * 128 + 128)
            outs, top, total = merge([part_ref[part, own, :, lanes]] + [recv1[part, d, :, lanes] for d in range(3)])
            acc1[part, b, 0:64] = outs[0]
            acc1[part, b, 64:128] = outs[1]
            acc1[part, b, 128:136] = jnp.concatenate([top, total, top, total], axis=0)
        start(part, 1)
    for part in range(3):
        for dist in (1, 2, 3):
            copies[part, 1, dist].wait_recv()
        own = pos[ORDERS[part][1]]
        outs, top, total = merge([acc1[part, own]] + [recv2[part, d] for d in range(3)])
        acc2[part, 0:64] = outs[0]
        acc2[part, 64:128] = outs[1]
        acc2[part, 128:136] = jnp.concatenate([top, total, top, total], axis=0)
        start(part, 2)
    mine[0] = att_ref[...]
    for part in range(3):
        for dist in (1, 2, 3):
            copies[part, 2, dist].wait_recv()
        outs, top, total = merge([acc2[part]] + [recv3[part, d] for d in range(3)])
        turned[part] = jnp.transpose(jnp.concatenate([outs[h] / total[h:h + 1] for h in range(2)], axis=0))
        rows = pl.ds(pl.multiple_of(pos[ORDERS[part][2]] * 32, 32), 32)
        mine[1, :, part * 128:part * 128 + 128] = turned[part, rows, :].astype(jnp.bfloat16)
    n_own = out_ref.shape[2]
    theirs = pl.ds(pl.multiple_of((1 - core) * n_own, n_own), n_own)
    last = pltpu.make_async_remote_copy(
        src_ref=mine.at[:, theirs], dst_ref=out_ref.at[core], send_sem=sib_send, recv_sem=sib_recv,
        device_id=device_of(pos, 1 - core), device_id_type=MESH)
    last.start()
    own_rows = pl.ds(pl.multiple_of(core * n_own, n_own), n_own)
    out_ref[core] = mine[:, own_rows]
    last.wait()
    for one in copies.values():
        one.wait_send()


def merge_parts(partial, att):
    f32, bf16 = jnp.float32, jnp.bfloat16
    n_rows, half = att.shape
    return pl.pallas_call(
        merge_kernel,
        out_shape=jax.ShapeDtypeStruct((2, 2, n_rows // 2, half), bf16),
        in_specs=[VMEM_SPEC] * 2,
        out_specs=VMEM_SPEC,
        scratch_shapes=[pltpu.VMEM((3, 3, 136, 512), f32), pltpu.VMEM((3, 4, 136, 128), f32),
                        pltpu.VMEM((3, 3, 136, 128), f32), pltpu.VMEM((3, 136, 128), f32),
                        pltpu.VMEM((3, 3, 136, 128), f32), pltpu.VMEM((3, 128, 128), f32),
                        pltpu.VMEM((2, n_rows, half), bf16),
                        pltpu.SemaphoreType.DMA((3, 3, 3)), pltpu.SemaphoreType.DMA((3, 3, 3)),
                        pltpu.SemaphoreType.DMA, pltpu.SemaphoreType.DMA],
        compiler_params=pltpu.CompilerParams(collective_id=2, has_side_effects=True),
        name="merge_parts",
    )(partial, att)


def solution(mesh):
    row_spec = P(("dp", "sp"), None)
    full_spec = P()

    def device_step(y_dec, memory, mem_len, norm_gain, self_wq, self_wk, self_wv, self_wo, cross_wq, cross_wk, cross_wv, cross_wo, mlp_gate, mlp_up, mlp_down):
        tq_dev, width = y_dec.shape
        tm_dev = memory.shape[0]
        sp = lax.axis_index("sp")
        chip = sp // 2
        n_valid = jnp.clip(mem_len[0] - chip * (2 * tm_dev), 0, 2 * tm_dev)
        info = jnp.stack([chip, sp % 2, n_valid, (n_valid + ROW_TILE - 1) // ROW_TILE]).astype(jnp.int32)
        chip_memory = swap_memory(memory).reshape(2 * tm_dev, width)
        keys, values = memory_kv(info, chip_memory, cross_wk, cross_wv)
        hidden = y_dec
        for layer in range(norm_gain.shape[0]):
            normed = rms_norm(hidden, norm_gain[layer])
            gathered = gather_rows(normed)
            att, qt = self_attention(info, gathered, layer, self_wq, self_wk, self_wv, cross_wq)
            partial = cross_attention(info, layer, qt, keys, values)
            merged = merge_parts(partial, att)
            merged = merged.transpose(1, 2, 0, 3).reshape(2, tq_dev, width)
            self_part = matmul(merged[0], self_wo[layer])
            cross_part = matmul(merged[1], cross_wo[layer])
            activated = (jax.nn.silu(matmul(normed, mlp_gate[layer])) * matmul(normed, mlp_up[layer])).astype(jnp.bfloat16)
            mlp_part = matmul(activated, mlp_down[layer])
            hidden = (hidden.astype(jnp.float32) + self_part + cross_part + mlp_part).astype(jnp.bfloat16)
        return hidden

    return jax.shard_map(device_step, mesh=mesh, in_specs=(row_spec, row_spec, P("dp")) + (full_spec,) * 12, out_specs=row_spec, check_vma=False)
```

```python
import functools
import math

import jax
import jax.numpy as jnp
from jax import lax
from jax.experimental import pallas as pl
from jax.experimental.pallas import tpu as pltpu
from jax.sharding import PartitionSpec as P

HEAD = 64
NORM_EPS = 1e-6
NEG_BIG = -1e30
MESH = pl.DeviceIdType.MESH
EXP_SCALE = HEAD ** -0.5 * math.log2(math.e)
ORDERS = ((0, 1, 2), (1, 2, 0), (2, 0, 1))
VMEM_SPEC = pl.BlockSpec(memory_space=pltpu.VMEM)
ROW_TILE = 512
LANES = 128
PART_ROWS = 136
PARTS = range(3)
NEAR_FIRST = (1, 3, 2)
FAR_FIRST = (2, 1, 3)
PHASE_SEMS = pltpu.SemaphoreType.DMA((3, 3, 3))
CHUNK_SEMS = pltpu.SemaphoreType.DMA((3, 4))


def in_hbm(array):
    return pltpu.with_memory_space_constraint(array, pltpu.HBM)


def matmul(left_mat, right_mat):
    return jnp.dot(left_mat, right_mat, preferred_element_type=jnp.float32)


def rms_norm(hidden, gain_vec):
    wide_vals = hidden.astype(jnp.float32)
    inv_rms = lax.rsqrt(jnp.mean(wide_vals * wide_vals, axis=-1, keepdims=True) + NORM_EPS)
    return (wide_vals * inv_rms * gain_vec.astype(jnp.float32)).astype(jnp.bfloat16)


def coords():
    sp = lax.axis_index("sp")
    return (sp // 32, (sp // 8) % 4, (sp // 2) % 4), sp % 2


def device_of(pos, core):
    return {"sp": ((pos[0] * 4 + pos[1]) * 4 + pos[2]) * 2 + core}


def shifted(pos, axis, dist):
    return tuple((c + dist) % 4 if i == axis else c for i, c in enumerate(pos))


def entry_barrier(pos, core):
    sem = pltpu.get_barrier_semaphore()
    for axis in PARTS:
        for dist in NEAR_FIRST:
            pl.semaphore_signal(sem, inc=1, device_id=device_of(shifted(pos, axis, dist), core), device_id_type=MESH)
    pl.semaphore_signal(sem, inc=1, device_id=device_of(pos, 1 - core), device_id_type=MESH)
    pl.semaphore_wait(sem, 10)


def gather_slice(ref, part, free, pos, core):
    idx = [part] + [slice(None) if axis in free else pos[axis] for axis in PARTS]
    return ref.at[tuple(idx) + (core,)]


GATHER_SEMS = [pltpu.SemaphoreType.DMA((3,)), PHASE_SEMS, PHASE_SEMS,
               CHUNK_SEMS, CHUNK_SEMS]


def run_gather(x_ref, out_ref, sems, pos, core, after_phase=None):
    local_sem, send_sem, recv_sem, sib_send, sib_recv = sems
    sibling = device_of(pos, 1 - core)

    def phase_copy(part, phase, dist):
        order = ORDERS[part]
        dst = gather_slice(out_ref, part, order[:phase], pos, core)
        return pltpu.make_async_remote_copy(
            src_ref=x_ref.at[part] if phase == 0 else dst, dst_ref=dst, send_sem=send_sem.at[part, phase, dist - 1],
            recv_sem=recv_sem.at[part, phase, dist - 1],
            device_id=device_of(shifted(pos, order[phase], dist), core), device_id_type=MESH)

    def sibling_copy(part, dist):
        order = ORDERS[part]
        ref = gather_slice(out_ref, part, order[:2], shifted(pos, order[2], 4 - dist), core)
        return pltpu.make_async_remote_copy(
            src_ref=ref, dst_ref=ref, send_sem=sib_send.at[part, dist], recv_sem=sib_recv.at[part, dist],
            device_id=sibling, device_id_type=MESH)

    local = [pltpu.make_async_copy(x_ref.at[p], gather_slice(out_ref, p, (), pos, core), local_sem.at[p])
             for p in PARTS]
    copies = {}
    for phase in PARTS:
        for part in PARTS:
            if phase == 1:
                local[part].wait()
            if phase > 0:
                for dist in NEAR_FIRST:
                    copies[part, phase - 1, dist].wait_recv()
            for dist in FAR_FIRST:
                copies[part, phase, dist] = phase_copy(part, phase, dist)
                copies[part, phase, dist].start()
            if phase == 0:
                local[part].start()
            if phase == 2:
                copies[part, 3, 0] = sibling_copy(part, 0)
                copies[part, 3, 0].start()
        if after_phase is not None:
            after_phase(phase)
    for dist in NEAR_FIRST:
        for part in PARTS:
            copies[part, 2, dist].wait_recv()
            copies[part, 3, dist] = sibling_copy(part, dist)
            copies[part, 3, dist].start()
    for part in PARTS:
        for dist in range(4):
            copies[part, 3, dist].wait_recv()
    for copy in copies.values():
        copy.wait_send()


def store_normed(x_ref, hidden, gain_vec):
    normed = rms_norm(hidden, gain_vec)
    third = x_ref.shape[2]
    for part in PARTS:
        x_ref[part] = normed[:, part * third:part * third + third]


def self_scratch(rows, width):
    bf16 = jnp.bfloat16
    half = width // 2
    n_rows = LANES * rows
    return [pltpu.VMEM((3, 4, 4, 4, 2, rows, width // 3), bf16), pltpu.VMEM((width, 4 * half), bf16),
            pltpu.VMEM((n_rows, half), bf16), pltpu.VMEM((n_rows, half), bf16),
            pltpu.VMEM((4, 4, 4, 2 * rows, half), bf16), pltpu.SemaphoreType.DMA((4,))]


def self_loads(layer, core, weights, w_ref, w_sem):
    half = w_ref.shape[1] // 4
    cols = pl.ds(pl.multiple_of(core * half, half), half)
    return [pltpu.make_async_copy(weight.at[layer, :, cols], w_ref.at[:, i * half:i * half + half], w_sem.at[i])
            for i, weight in enumerate(weights)]


def self_body(pos, h_ref, w_ref, k_ref, v_ref, q_ref, att_ref, qt_ref):
    half = k_ref.shape[1]
    n_query = att_ref.shape[0]
    chip = (pos[0] * 4 + pos[1]) * 4 + pos[2]

    def rows_cat(z, y, x):
        return jnp.concatenate([h_ref[p, z, y, x].reshape(n_query, -1) for p in PARTS], axis=1)

    def key_tile(z, carry):
        rows = jnp.concatenate([rows_cat(z, y, x) for y in range(4) for x in range(4)], axis=0)
        at = pl.ds(pl.multiple_of(z * ROW_TILE, ROW_TILE), ROW_TILE)
        made = matmul(rows, w_ref[:, :3 * half]).astype(jnp.bfloat16)
        k_ref[at, :] = made[:, :half]
        v_ref[at, :] = made[:, half:2 * half]
        q_ref[z] = made[:, 2 * half:].reshape(4, 4, n_query, half)
        return carry

    lax.fori_loop(0, 4, key_tile, 0)

    for part in PARTS:
        cols = slice(part * LANES, part * LANES + LANES)

        def query_tile(a, carry, part=part, cols=cols):
            order = ORDERS[part]
            for b in range(4):
                blocks = []
                for c in range(4):
                    at = [None] * 3
                    at[order[0]], at[order[1]], at[order[2]] = a, b, c
                    blocks.append(q_ref[at[0], at[1], at[2], :, cols])
                qt_ref[part, a * 4 + b] = jnp.transpose(jnp.concatenate(blocks, axis=0))
            return carry

        lax.fori_loop(0, 4, query_tile, 0)

    query = matmul(rows_cat(*pos), w_ref[:, 3 * half:]).astype(jnp.bfloat16)
    n_keys = k_ref.shape[0]
    low = lax.broadcasted_iota(jnp.int32, (n_query, LANES), 1) < HEAD
    key_pos = lax.broadcasted_iota(jnp.int32, (2 * n_query, n_keys), 1)
    query_pos = chip * n_query + lax.broadcasted_iota(jnp.int32, (2 * n_query, n_keys), 0) % n_query
    causal = key_pos <= query_pos
    zero = jnp.zeros((n_query, LANES), jnp.bfloat16)
    for part in PARTS:
        cols = slice(part * LANES, part * LANES + LANES)
        q_pair = query[:, cols]
        q_two = jnp.concatenate([jnp.where(low, q_pair, zero), jnp.where(low, zero, q_pair)], axis=0)
        s = lax.dot_general(q_two, k_ref[:, cols], (((1,), (1,)), ((), ())), preferred_element_type=jnp.float32)
        s = jnp.where(causal, s, NEG_BIG)
        top = jnp.max(s, axis=1, keepdims=True)
        w = jnp.exp2((s - top) * EXP_SCALE)
        total = jnp.sum(w, axis=1, keepdims=True)
        o = matmul(w.astype(jnp.bfloat16), v_ref[:, cols]) / total
        att_ref[:, cols] = jnp.where(low, o[:n_query], o[n_query:]).astype(jnp.bfloat16)


SPREAD = ((0, 64), (64, 64), (LANES, LANES))
SPREAD_ROWS = 256


def first_kernel(y_ref, gain_ref, mem_ref, wk, wv, cq, wq, att_ref, qt_ref, mem_out,
                 x_ref, h_ref, w_ref, k_ref, v_ref, q_ref, w_sem,
                 local_sem, ex_send, ex_recv, fw_send, fw_recv, *sems):
    pos, core = coords()
    loads = self_loads(0, core, (wk, wv, cq, wq), w_ref, w_sem)
    for load in loads:
        load.start()
    z = pos[0]
    own = pltpu.make_async_copy(mem_ref.at[jnp.minimum(z, 2)], mem_out.at[jnp.minimum(z, 2), core], local_sem)
    entry_barrier(pos, core)
    sibling = device_of(pos, 1 - core)

    def spread_copy(dist, piece):
        to = (z + dist) % 4
        start, size = SPREAD[piece]
        rows = pl.ds(start, size)
        return pltpu.make_async_remote_copy(
            src_ref=mem_ref.at[to, rows], dst_ref=mem_out.at[jnp.minimum(z, 2), core, rows],
            send_sem=ex_send.at[piece, dist - 1], recv_sem=ex_recv.at[piece, dist - 1],
            device_id=device_of(shifted(pos, 0, dist), core), device_id_type=MESH)

    def forward_copy(dist, piece):
        at = jnp.minimum((z + 4 - dist) % 4, 2)
        start, size = SPREAD[piece]
        rows = pl.ds(start, size)
        src = mem_ref.at[at, rows] if dist == 0 else mem_out.at[at, core, rows]
        return pltpu.make_async_remote_copy(
            src_ref=src, dst_ref=mem_out.at[at, core, rows], send_sem=fw_send.at[piece, dist],
            recv_sem=fw_recv.at[piece, dist], device_id=sibling, device_id_type=MESH)

    def spread(piece):
        @pl.when(z < 3)
        def _():
            for dist in FAR_FIRST:
                spread_copy(dist, piece).start()

    def forward(piece):
        @pl.when(z < 3)
        def _():
            forward_copy(0, piece).start()
        for dist in NEAR_FIRST:
            @pl.when((z + 4 - dist) % 4 < 3)
            def _(dist=dist):
                spread_copy(dist, piece).wait_recv()
                forward_copy(dist, piece).start()

    @pl.when(z < 3)
    def _():
        own.start()
    store_normed(x_ref, y_ref[...], gain_ref[0:1, :])
    run_gather(x_ref, h_ref, sems, pos, core, after_phase=spread)
    for load in loads:
        load.wait()
    for piece in range(2):
        forward(piece)
    self_body(pos, h_ref, w_ref, k_ref, v_ref, q_ref, att_ref, qt_ref)
    forward(2)

    @pl.when(z < 3)
    def _():
        own.wait()
        for piece in PARTS:
            for dist in NEAR_FIRST:
                spread_copy(dist, piece).wait_send()
    for piece in PARTS:
        for dist in range(4):
            @pl.when((z + 4 - dist) % 4 < 3)
            def _(dist=dist, piece=piece):
                forward_copy(dist, piece).wait()


def att_shapes(rows, width):
    return [jax.ShapeDtypeStruct((2 * rows, width // 2), jnp.bfloat16),
            jax.ShapeDtypeStruct((3, 16, LANES, LANES), jnp.bfloat16)]


HBM_SPEC = pl.BlockSpec(memory_space=pltpu.HBM)


def first_layer(y_dec, norm_gain, memory, *weights):
    rows, width = y_dec.shape
    tm_dev = memory.shape[0]
    return pl.pallas_call(
        first_kernel,
        out_shape=att_shapes(rows, width) + [jax.ShapeDtypeStruct((3, 2, tm_dev // 4, width), memory.dtype)],
        in_specs=[VMEM_SPEC] * 2 + [HBM_SPEC] * 5,
        out_specs=[VMEM_SPEC] * 3,
        scratch_shapes=[pltpu.VMEM((3, rows, width // 3), jnp.bfloat16)] + self_scratch(rows, width)
        + [pltpu.SemaphoreType.DMA] + [pltpu.SemaphoreType.DMA((3, 3))] * 2 + [CHUNK_SEMS] * 2
        + GATHER_SEMS,
        compiler_params=pltpu.CompilerParams(collective_id=0, has_side_effects=True,
                                             vmem_limit_bytes=24 * 1024 * 1024),
        name="first_layer",
    )(y_dec, norm_gain, in_hbm(memory.reshape(4, tm_dev // 4, width)), *map(in_hbm, weights))


def kv_kernel(info_ref, m_ref, wk_ref, wv_ref, k_ref, vt_ref):
    @pl.when(pl.program_id(0) < info_ref[3])
    def _():
        rows = m_ref[...]
        half = wk_ref.shape[2]
        for layer in range(wk_ref.shape[0]):
            both = matmul(rows, jnp.concatenate([wk_ref[layer], wv_ref[layer]], axis=1)).astype(jnp.bfloat16)
            k_ref[layer] = both[:, :half]
            vt_ref[layer] = jnp.transpose(both[:, half:])


def memory_kv(info, chip_memory, wk, wv):
    n_rows, width = chip_memory.shape
    half = width // 2
    layers = wk.shape[0]
    w_spec = pl.BlockSpec((layers, width, half), lambda t, info: (0, 0, info[1]))
    return pl.pallas_call(
        kv_kernel,
        grid_spec=pltpu.PrefetchScalarGridSpec(
            num_scalar_prefetch=1,
            grid=(n_rows // ROW_TILE,),
            in_specs=[pl.BlockSpec((ROW_TILE, width), lambda t, info: (t, 0)), w_spec, w_spec],
            out_specs=[pl.BlockSpec((layers, ROW_TILE, half), lambda t, info: (0, t, 0)),
                       pl.BlockSpec((layers, half, ROW_TILE), lambda t, info: (0, 0, t))],
        ),
        out_shape=[jax.ShapeDtypeStruct((layers, n_rows, half), jnp.bfloat16),
                   jax.ShapeDtypeStruct((layers, half, n_rows), jnp.bfloat16)],
        compiler_params=pltpu.CompilerParams(vmem_limit_bytes=24 * 1024 * 1024),
        name="memory_kv",
    )(info, chip_memory, in_hbm(wk), in_hbm(wv))


def spread_start(chip, from_z, from_core):
    return ((from_z * 16 + chip % 16) * 2 + from_core) * 4 * SPREAD_ROWS + chip // 16 * SPREAD_ROWS


def cross_kernel(info_ref, qt_ref, k_ref, vt_ref, out_ref, bias_ref, q0_ref, q1_ref, s0_ref, s1_ref):
    n_tiles = info_ref[3]
    n_q = q0_ref.shape[1]
    n_pairs = 3 * 4
    chip = info_ref[0]
    row = lax.broadcasted_iota(jnp.int32, (SPREAD_ROWS, LANES), 0)
    for block in range(bias_ref.shape[0] // SPREAD_ROWS):
        start = spread_start(chip, block // 2, block % 2)
        bias_ref[block * SPREAD_ROWS:(block + 1) * SPREAD_ROWS, :] = jnp.where(
            row < info_ref[2] - start, 0.0, NEG_BIG).astype(jnp.bfloat16)
    for ref in (q0_ref, q1_ref):
        lane_one = lax.broadcasted_iota(jnp.int32, (LANES, n_q), 0) == 0
        ref[LANES:256, :] = jnp.where(lane_one, 1.0, 0.0).astype(jnp.bfloat16)
        ref[0:LANES, :] = jnp.zeros((LANES, n_q), jnp.bfloat16)

    def set_query(ref, head, pair):
        part, tile = pair // 4, pair % 4
        rows = slice(head * HEAD, head * HEAD + HEAD)
        for i in range(4):
            ref[rows, i * LANES:i * LANES + LANES] = qt_ref[part, tile * 4 + i, rows, :]

    def rows_of(t):
        return pl.ds(pl.multiple_of(t * ROW_TILE, ROW_TILE), ROW_TILE)

    def fold(op, vals):
        return op(vals.reshape(ROW_TILE // 8, 8, n_q), axis=0)

    def score(t, q_ref, s_ref, pair, top):
        lanes = pl.ds(pl.multiple_of((pair // 4) * LANES, LANES), LANES)
        keys = jnp.concatenate([k_ref[rows_of(t), lanes], bias_ref[rows_of(t), :]], axis=1)
        s = matmul(keys, q_ref[...])
        s_ref[rows_of(t), :] = s
        return jnp.maximum(top, fold(jnp.max, s))

    def weigh(t, s_ref, pair, head, shift, total):
        w = jnp.exp2(s_ref[rows_of(t), :] * EXP_SCALE - shift)
        vals = pl.ds(pl.multiple_of((pair // 4) * LANES + head * HEAD, HEAD), HEAD)
        out_ref[pair // 4, pair % 4, head * HEAD:head * HEAD + HEAD, :] += matmul(
            vt_ref[vals, rows_of(t)], w.astype(jnp.bfloat16))
        return total + fold(jnp.sum, w)

    low_top = jnp.full((8, n_q), NEG_BIG, jnp.float32)
    no_sum = jnp.zeros((8, n_q), jnp.float32)

    def shift_of(top):
        return jnp.max(top, axis=0, keepdims=True) * EXP_SCALE

    def pair_step(pair, top0):
        part, tile = pair // 4, pair % 4
        out_ref[part, tile, 0:LANES, :] = jnp.zeros((LANES, n_q), jnp.float32)
        shift0 = shift_of(top0)
        set_query(q1_ref, 1, pair)

        def first(t, carry):
            top, total = carry
            return score(t, q1_ref, s1_ref, pair, top), weigh(t, s0_ref, pair, 0, shift0, total)

        top1, total0 = lax.fori_loop(0, n_tiles, first, (low_top, no_sum))
        shift1 = shift_of(top1)
        after = jnp.minimum(pair + 1, n_pairs - 1)
        set_query(q0_ref, 0, after)

        def second(t, carry):
            top, total = carry
            return score(t, q0_ref, s0_ref, after, top), weigh(t, s1_ref, pair, 1, shift1, total)

        next_top, total1 = lax.fori_loop(0, n_tiles, second, (low_top, no_sum))
        sums = [jnp.sum(v, axis=0, keepdims=True) for v in (total0, total1)]
        out_ref[part, tile, LANES:PART_ROWS, :] = jnp.concatenate([shift0, shift1] + sums + [shift0, shift1] + sums, axis=0)
        return next_top

    set_query(q0_ref, 0, 0)
    top0 = lax.fori_loop(0, n_tiles, lambda t, top: score(t, q0_ref, s0_ref, 0, top), low_top)
    lax.fori_loop(0, n_pairs, pair_step, top0)


def cross_attention(info, layer, qt, keys, values):
    n_rows, half = keys.shape[1:]
    return pl.pallas_call(
        cross_kernel,
        grid_spec=pltpu.PrefetchScalarGridSpec(
            num_scalar_prefetch=1,
            grid=(1,),
            in_specs=[pl.BlockSpec(qt.shape, lambda i, info: (0, 0, 0, 0)),
                      pl.BlockSpec((None, n_rows, half), lambda i, info: (layer, 0, 0)),
                      pl.BlockSpec((None, half, n_rows), lambda i, info: (layer, 0, 0))],
            out_specs=pl.BlockSpec((3, 4, PART_ROWS, ROW_TILE), lambda i, info: (0, 0, 0, 0)),
            scratch_shapes=[pltpu.VMEM((n_rows, LANES), jnp.bfloat16)]
            + [pltpu.VMEM((256, ROW_TILE), jnp.bfloat16)] * 2 + [pltpu.VMEM((n_rows, ROW_TILE), jnp.float32)] * 2,
        ),
        out_shape=jax.ShapeDtypeStruct((3, 4, PART_ROWS, ROW_TILE), jnp.float32),
        compiler_params=pltpu.CompilerParams(vmem_limit_bytes=26 * 1024 * 1024),
        name="cross_attention",
    )(info, qt, keys, values)


def merge(pieces):
    tops = [p[LANES:130] for p in pieces]
    sums = [p[130:132] for p in pieces]
    top = functools.reduce(jnp.maximum, tops)
    fixes = [jnp.exp2(t - top) for t in tops]
    total = functools.reduce(jnp.add, [f * s for f, s in zip(fixes, sums)])
    outs = []
    for head in range(2):
        rows = slice(head * HEAD, head * HEAD + HEAD)
        outs.append(functools.reduce(jnp.add, [p[rows] * f[head:head + 1] for p, f in zip(pieces, fixes)]))
    return outs, top, total


def store_merged(ref, outs, top, total):
    ref[0:64] = outs[0]
    ref[64:LANES] = outs[1]
    ref[LANES:PART_ROWS] = jnp.concatenate([top, total, top, total], axis=0)


def finish_kernel(layer, last, part_ref, att_ref, hid_ref, gain_ref, w1_hbm, w3_hbm, w2_hbm, wo_hbm, co_hbm, *refs):
    if not last:
        next_weights, refs = refs[:4], refs[4:]
    n_out = 1 if last else 3
    outs_refs, refs = refs[:n_out], refs[n_out:]
    (w1, w3, w2, wo, co, recv1, acc1, recv2, acc2, recv3, turned, mine, full, x_ref,
     w_sem, send_sem, recv_sem, sib_send, sib_recv) = refs[:19]
    pos, core = coords()
    loads = [pltpu.make_async_copy(src.at[layer], dst, w_sem.at[i]) for i, (src, dst) in enumerate(
        ((w1_hbm, w1), (w3_hbm, w3), (w2_hbm, w2), (wo_hbm, wo), (co_hbm, co)))]
    if not last:
        h_ref, w_ref, k_ref, v_ref, q_ref, nw_sem = refs[19:25]
        next_loads = self_loads(layer + 1, core, next_weights, w_ref, nw_sem)
        loads += next_loads
    for load in loads:
        load.start()
    entry_barrier(pos, core)

    def copy(part, phase, dist):
        axis = ORDERS[part][phase]
        peer = shifted(pos, axis, dist)
        src, dst = ((part_ref.at[part, peer[axis]], recv1.at[part, dist - 1]),
                    (acc1.at[part, peer[axis]], recv2.at[part, dist - 1]),
                    (acc2.at[part], recv3.at[part, dist - 1]))[phase]
        return pltpu.make_async_remote_copy(
            src_ref=src, dst_ref=dst, send_sem=send_sem.at[part, phase, dist - 1],
            recv_sem=recv_sem.at[part, phase, dist - 1], device_id=device_of(peer, core), device_id_type=MESH)

    copies = {}

    def start(part, phase):
        for dist in FAR_FIRST:
            copies[part, phase, dist] = copy(part, phase, dist)
            copies[part, phase, dist].start()

    for part in PARTS:
        start(part, 0)

    hidden = hid_ref[...]
    normed = rms_norm(hidden, gain_ref[layer:layer + 1, :])
    for load in loads[:3]:
        load.wait()
    activated = (jax.nn.silu(matmul(normed, w1[...])) * matmul(normed, w3[...])).astype(jnp.bfloat16)
    mlp_part = matmul(activated, w2[...])

    for part in PARTS:
        for dist in NEAR_FIRST:
            copies[part, 0, dist].wait_recv()
        own = pos[ORDERS[part][0]]
        for b in range(4):
            lanes = slice(b * LANES, b * LANES + LANES)
            merged = merge([part_ref[part, own, :, lanes]] + [recv1[part, d, :, lanes] for d in PARTS])
            store_merged(acc1.at[part, b], *merged)
        start(part, 1)
    for part in PARTS:
        for dist in NEAR_FIRST:
            copies[part, 1, dist].wait_recv()
        own = pos[ORDERS[part][1]]
        store_merged(acc2.at[part], *merge([acc1[part, own]] + [recv2[part, d] for d in PARTS]))
        start(part, 2)
    mine[0] = att_ref[...]
    for part in PARTS:
        for dist in NEAR_FIRST:
            copies[part, 2, dist].wait_recv()
        outs, top, total = merge([acc2[part]] + [recv3[part, d] for d in PARTS])
        turned[part] = jnp.transpose(jnp.concatenate([outs[h] / total[h:h + 1] for h in range(2)], axis=0))
        rows = pl.ds(pl.multiple_of(pos[ORDERS[part][2]] * 32, 32), 32)
        mine[1, :, part * LANES:part * LANES + LANES] = turned[part, rows, :].astype(jnp.bfloat16)
    n_own = hid_ref.shape[0]
    theirs = pl.ds(pl.multiple_of((1 - core) * n_own, n_own), n_own)
    last_copy = pltpu.make_async_remote_copy(
        src_ref=mine.at[:, theirs], dst_ref=full.at[core], send_sem=sib_send, recv_sem=sib_recv,
        device_id=device_of(pos, 1 - core), device_id_type=MESH)
    last_copy.start()
    own_rows = pl.ds(pl.multiple_of(core * n_own, n_own), n_own)
    full[core] = mine[:, own_rows]
    for load in loads[3:5]:
        load.wait()
    last_copy.wait()
    parts = []
    for i, weight in enumerate((wo, co)):
        parts.append(matmul(jnp.concatenate([full[0, i], full[1, i]], axis=1), weight[...]))
    result = (hidden.astype(jnp.float32) + parts[0] + parts[1] + mlp_part).astype(jnp.bfloat16)
    outs_refs[0][...] = result
    if not last:
        store_normed(x_ref, result, gain_ref[layer + 1:layer + 2, :])
        run_gather(x_ref, h_ref, refs[25:], pos, core)
        for load in next_loads:
            load.wait()
        self_body(pos, h_ref, w_ref, k_ref, v_ref, q_ref, outs_refs[1], outs_refs[2])
    for one in copies.values():
        one.wait_send()


def finish_layer(layer, last, partial, att, hidden, gain, w1, w3, w2, wo, co, *next_weights):
    f32, bf16 = jnp.float32, jnp.bfloat16
    n_rows, half = att.shape
    rows, width = hidden.shape
    ff = w1.shape[2]
    third = width // 3
    out_shape = [jax.ShapeDtypeStruct(hidden.shape, bf16)]
    if not last:
        out_shape += att_shapes(rows, width)
    return pl.pallas_call(
        functools.partial(finish_kernel, layer, last),
        out_shape=out_shape,
        in_specs=[VMEM_SPEC] * 4 + [HBM_SPEC] * (5 + len(next_weights)),
        out_specs=[VMEM_SPEC] * len(out_shape),
        scratch_shapes=[pltpu.VMEM((width, ff), bf16), pltpu.VMEM((width, ff), bf16), pltpu.VMEM((ff, width), bf16),
                        pltpu.VMEM((width, width), bf16), pltpu.VMEM((width, width), bf16),
                        pltpu.VMEM((3, 3, PART_ROWS, ROW_TILE), f32), pltpu.VMEM((3, 4, PART_ROWS, LANES), f32),
                        pltpu.VMEM((3, 3, PART_ROWS, LANES), f32), pltpu.VMEM((3, PART_ROWS, LANES), f32),
                        pltpu.VMEM((3, 3, PART_ROWS, LANES), f32), pltpu.VMEM((3, LANES, LANES), f32),
                        pltpu.VMEM((2, n_rows, half), bf16), pltpu.VMEM((2, 2, rows, half), bf16),
                        pltpu.VMEM((3, rows, third), bf16),
                        pltpu.SemaphoreType.DMA((5,)),
                        PHASE_SEMS, PHASE_SEMS,
                        pltpu.SemaphoreType.DMA, pltpu.SemaphoreType.DMA]
        + ([] if last else self_scratch(rows, width) + GATHER_SEMS),
        compiler_params=pltpu.CompilerParams(collective_id=1 + layer, has_side_effects=True,
                                             vmem_limit_bytes=32 * 1024 * 1024),
        name="finish_layer",
    )(partial, att, hidden, gain, *map(in_hbm, (w1, w3, w2, wo, co) + next_weights))


def solution(mesh):
    row_spec = P(("dp", "sp"), None)
    full_spec = P()

    def device_step(y_dec, memory, mem_len, norm_gain, self_wq, self_wk, self_wv, self_wo, cross_wq, cross_wk, cross_wv, cross_wo, mlp_gate, mlp_up, mlp_down):
        tq_dev, width = y_dec.shape
        tm_dev = memory.shape[0]
        sp = lax.axis_index("sp")
        chip = sp // 2
        tiles = [jnp.where(spread_start(chip, z, 0) < mem_len[0], 1, 0) for z in PARTS]
        info = jnp.stack([chip, sp % 2, mem_len[0], sum(tiles)]).astype(jnp.int32)
        weights = (self_wk, self_wv, cross_wq, self_wq)
        att, qt, rows = first_layer(y_dec, norm_gain, memory, *weights)
        keys, values = memory_kv(info, rows.reshape(3 * tm_dev // 2, width), cross_wk, cross_wv)
        hidden = y_dec
        layers = norm_gain.shape[0]
        for layer in range(layers):
            partial = cross_attention(info, layer, qt, keys, values)
            last = layer == layers - 1
            out = finish_layer(layer, last, partial, att, hidden, norm_gain, mlp_gate, mlp_up, mlp_down, self_wo,
                               cross_wo, *(() if last else weights))
            hidden = out[0]
            if not last:
                att, qt = out[1:]
        return hidden

    return jax.shard_map(device_step, mesh=mesh, in_specs=(row_spec, row_spec, P("dp")) + (full_spec,) * 12, out_specs=row_spec, check_vma=False)
```

```python
import functools
import math

import jax
import jax.numpy as jnp
from jax import lax
from jax.experimental import pallas as pl
from jax.experimental.pallas import tpu as pltpu
from jax.sharding import PartitionSpec as P

HEAD = 64
NORM_EPS = 1e-6
NEG_BIG = -1e30
MESH = pl.DeviceIdType.MESH
EXP_SCALE = HEAD ** -0.5 * math.log2(math.e)
ORDERS = ((0, 1, 2), (1, 2, 0), (2, 0, 1))
VMEM_SPEC = pl.BlockSpec(memory_space=pltpu.VMEM)
ROW_TILE = 512
LANES = 128
PART_ROWS = 136
PARTS = range(3)
NEAR_FIRST = (1, 3, 2)
FAR_FIRST = (2, 1, 3)
PHASE_SEMS = pltpu.SemaphoreType.DMA((3, 3, 3))
CUT_SEMS = pltpu.SemaphoreType.DMA((3, 4, 3))
CHUNK_SEMS = pltpu.SemaphoreType.DMA((3, 4))


def in_hbm(array):
    return pltpu.with_memory_space_constraint(array, pltpu.HBM)


def matmul(left_mat, right_mat):
    return jnp.dot(left_mat, right_mat, preferred_element_type=jnp.float32)


def rms_norm(hidden, gain_vec):
    wide_vals = hidden.astype(jnp.float32)
    inv_rms = lax.rsqrt(jnp.mean(wide_vals * wide_vals, axis=-1, keepdims=True) + NORM_EPS)
    return (wide_vals * inv_rms * gain_vec.astype(jnp.float32)).astype(jnp.bfloat16)


def coords():
    sp = lax.axis_index("sp")
    return (sp // 32, (sp // 8) % 4, (sp // 2) % 4), sp % 2


def device_of(pos, core):
    return {"sp": ((pos[0] * 4 + pos[1]) * 4 + pos[2]) * 2 + core}


def shifted(pos, axis, dist):
    return tuple((c + dist) % 4 if i == axis else c for i, c in enumerate(pos))


def entry_barrier(pos, core):
    sem = pltpu.get_barrier_semaphore()
    for axis in PARTS:
        for dist in NEAR_FIRST:
            pl.semaphore_signal(sem, inc=1, device_id=device_of(shifted(pos, axis, dist), core), device_id_type=MESH)
    pl.semaphore_signal(sem, inc=1, device_id=device_of(pos, 1 - core), device_id_type=MESH)
    pl.semaphore_wait(sem, 10)


def gather_slice(ref, part, free, pos, core):
    idx = [part] + [slice(None) if axis in free else pos[axis] for axis in PARTS]
    return ref.at[tuple(idx) + (core,)]


GATHER_SEMS = [pltpu.SemaphoreType.DMA((3,)), PHASE_SEMS, PHASE_SEMS,
               CHUNK_SEMS, CHUNK_SEMS]


def run_gather(x_ref, out_ref, sems, pos, core, after_phase=None):
    local_sem, send_sem, recv_sem, sib_send, sib_recv = sems
    sibling = device_of(pos, 1 - core)

    def phase_copy(part, phase, dist):
        order = ORDERS[part]
        dst = gather_slice(out_ref, part, order[:phase], pos, core)
        return pltpu.make_async_remote_copy(
            src_ref=x_ref.at[part] if phase == 0 else dst, dst_ref=dst, send_sem=send_sem.at[part, phase, dist - 1],
            recv_sem=recv_sem.at[part, phase, dist - 1],
            device_id=device_of(shifted(pos, order[phase], dist), core), device_id_type=MESH)

    def sibling_copy(part, dist):
        order = ORDERS[part]
        ref = gather_slice(out_ref, part, order[:2], shifted(pos, order[2], 4 - dist), core)
        return pltpu.make_async_remote_copy(
            src_ref=ref, dst_ref=ref, send_sem=sib_send.at[part, dist], recv_sem=sib_recv.at[part, dist],
            device_id=sibling, device_id_type=MESH)

    local = [pltpu.make_async_copy(x_ref.at[p], gather_slice(out_ref, p, (), pos, core), local_sem.at[p])
             for p in PARTS]
    copies = {}
    for phase in PARTS:
        for part in PARTS:
            if phase == 1:
                local[part].wait()
            if phase > 0:
                for dist in NEAR_FIRST:
                    copies[part, phase - 1, dist].wait_recv()
            for dist in FAR_FIRST:
                copies[part, phase, dist] = phase_copy(part, phase, dist)
                copies[part, phase, dist].start()
            if phase == 0:
                local[part].start()
            if phase == 2:
                copies[part, 3, 0] = sibling_copy(part, 0)
                copies[part, 3, 0].start()
        if after_phase is not None:
            after_phase(phase)
    for dist in NEAR_FIRST:
        for part in PARTS:
            copies[part, 2, dist].wait_recv()
            copies[part, 3, dist] = sibling_copy(part, dist)
            copies[part, 3, dist].start()
    for part in PARTS:
        for dist in range(4):
            copies[part, 3, dist].wait_recv()
    for copy in copies.values():
        copy.wait_send()


def store_normed(x_ref, hidden, gain_vec):
    normed = rms_norm(hidden, gain_vec)
    third = x_ref.shape[2]
    for part in PARTS:
        x_ref[part] = normed[:, part * third:part * third + third]


def self_scratch(rows, width):
    bf16 = jnp.bfloat16
    half = width // 2
    n_rows = LANES * rows
    return [pltpu.VMEM((3, 4, 4, 4, 2, rows, width // 3), bf16), pltpu.VMEM((width, 4 * half), bf16),
            pltpu.VMEM((n_rows, half), bf16), pltpu.VMEM((n_rows, half), bf16),
            pltpu.VMEM((4, 4, 4, 2 * rows, half), bf16), pltpu.SemaphoreType.DMA((4,))]


def half_loads(layer, core, weights, w_ref, w_sem):
    half = w_ref.shape[1] // len(weights)
    cols = pl.ds(pl.multiple_of(core * half, half), half)
    return [pltpu.make_async_copy(weight.at[layer, :, cols], w_ref.at[:, i * half:i * half + half], w_sem.at[i])
            for i, weight in enumerate(weights)]


def self_body(pos, h_ref, w_ref, k_ref, v_ref, q_ref, att_ref, qt_ref):
    half = k_ref.shape[1]
    n_query = att_ref.shape[0]
    chip = (pos[0] * 4 + pos[1]) * 4 + pos[2]

    def rows_cat(z, y, x):
        return jnp.concatenate([h_ref[p, z, y, x].reshape(n_query, -1) for p in PARTS], axis=1)

    def key_tile(z, carry):
        rows = jnp.concatenate([rows_cat(z, y, x) for y in range(4) for x in range(4)], axis=0)
        at = pl.ds(pl.multiple_of(z * ROW_TILE, ROW_TILE), ROW_TILE)
        made = matmul(rows, w_ref[:, :3 * half]).astype(jnp.bfloat16)
        k_ref[at, :] = made[:, :half]
        v_ref[at, :] = made[:, half:2 * half]
        q_ref[z] = made[:, 2 * half:].reshape(4, 4, n_query, half)
        return carry

    lax.fori_loop(0, 4, key_tile, 0)

    for part in PARTS:
        cols = slice(part * LANES, part * LANES + LANES)

        def query_tile(a, carry, part=part, cols=cols):
            order = ORDERS[part]
            for b in range(4):
                blocks = []
                for c in range(4):
                    at = [None] * 3
                    at[order[0]], at[order[1]], at[order[2]] = a, b, c
                    blocks.append(q_ref[at[0], at[1], at[2], :, cols])
                qt_ref[part, a * 4 + b] = jnp.transpose(jnp.concatenate(blocks, axis=0))
            return carry

        lax.fori_loop(0, 4, query_tile, 0)

    query = matmul(rows_cat(*pos), w_ref[:, 3 * half:]).astype(jnp.bfloat16)
    n_keys = k_ref.shape[0]
    low = lax.broadcasted_iota(jnp.int32, (n_query, LANES), 1) < HEAD
    key_pos = lax.broadcasted_iota(jnp.int32, (2 * n_query, n_keys), 1)
    query_pos = chip * n_query + lax.broadcasted_iota(jnp.int32, (2 * n_query, n_keys), 0) % n_query
    causal = key_pos <= query_pos
    zero = jnp.zeros((n_query, LANES), jnp.bfloat16)
    for part in PARTS:
        cols = slice(part * LANES, part * LANES + LANES)
        q_pair = query[:, cols]
        q_two = jnp.concatenate([jnp.where(low, q_pair, zero), jnp.where(low, zero, q_pair)], axis=0)
        s = lax.dot_general(q_two, k_ref[:, cols], (((1,), (1,)), ((), ())), preferred_element_type=jnp.float32)
        s = jnp.where(causal, s, NEG_BIG)
        top = jnp.max(s, axis=1, keepdims=True)
        w = jnp.exp2((s - top) * EXP_SCALE)
        total = jnp.sum(w, axis=1, keepdims=True)
        o = matmul(w.astype(jnp.bfloat16), v_ref[:, cols]) / total
        att_ref[:, cols] = jnp.where(low, o[:n_query], o[n_query:]).astype(jnp.bfloat16)


SPREAD = ((0, 64), (64, 64), (LANES, LANES))
SPREAD_ROWS = 256


def first_kernel(y_ref, gain_ref, mem_ref, wk, wv, cq, wq, att_ref, qt_ref, mem_out,
                 x_ref, h_ref, w_ref, k_ref, v_ref, q_ref, w_sem,
                 local_sem, ex_send, ex_recv, fw_send, fw_recv, *sems):
    pos, core = coords()
    loads = half_loads(0, core, (wk, wv, cq, wq), w_ref, w_sem)
    for load in loads:
        load.start()
    z = pos[0]
    own = pltpu.make_async_copy(mem_ref.at[jnp.minimum(z, 2)], mem_out.at[jnp.minimum(z, 2), core], local_sem)
    entry_barrier(pos, core)
    sibling = device_of(pos, 1 - core)

    def spread_copy(dist, piece):
        to = (z + dist) % 4
        start, size = SPREAD[piece]
        rows = pl.ds(start, size)
        return pltpu.make_async_remote_copy(
            src_ref=mem_ref.at[to, rows], dst_ref=mem_out.at[jnp.minimum(z, 2), core, rows],
            send_sem=ex_send.at[piece, dist - 1], recv_sem=ex_recv.at[piece, dist - 1],
            device_id=device_of(shifted(pos, 0, dist), core), device_id_type=MESH)

    def forward_copy(dist, piece):
        at = jnp.minimum((z + 4 - dist) % 4, 2)
        start, size = SPREAD[piece]
        rows = pl.ds(start, size)
        src = mem_ref.at[at, rows] if dist == 0 else mem_out.at[at, core, rows]
        return pltpu.make_async_remote_copy(
            src_ref=src, dst_ref=mem_out.at[at, core, rows], send_sem=fw_send.at[piece, dist],
            recv_sem=fw_recv.at[piece, dist], device_id=sibling, device_id_type=MESH)

    def spread(piece):
        @pl.when(z < 3)
        def _():
            for dist in FAR_FIRST:
                spread_copy(dist, piece).start()

    def forward(piece):
        @pl.when(z < 3)
        def _():
            forward_copy(0, piece).start()
        for dist in NEAR_FIRST:
            @pl.when((z + 4 - dist) % 4 < 3)
            def _(dist=dist):
                spread_copy(dist, piece).wait_recv()
                forward_copy(dist, piece).start()

    @pl.when(z < 3)
    def _():
        own.start()
    store_normed(x_ref, y_ref[...], gain_ref[0:1, :])
    run_gather(x_ref, h_ref, sems, pos, core, after_phase=spread)
    for load in loads:
        load.wait()
    for piece in range(2):
        forward(piece)
    self_body(pos, h_ref, w_ref, k_ref, v_ref, q_ref, att_ref, qt_ref)
    forward(2)

    @pl.when(z < 3)
    def _():
        own.wait()
        for piece in PARTS:
            for dist in NEAR_FIRST:
                spread_copy(dist, piece).wait_send()
    for piece in PARTS:
        for dist in range(4):
            @pl.when((z + 4 - dist) % 4 < 3)
            def _(dist=dist, piece=piece):
                forward_copy(dist, piece).wait()


def att_shapes(rows, width):
    return [jax.ShapeDtypeStruct((2 * rows, width // 2), jnp.bfloat16),
            jax.ShapeDtypeStruct((3, 16, LANES, LANES), jnp.bfloat16)]


HBM_SPEC = pl.BlockSpec(memory_space=pltpu.HBM)


def first_layer(y_dec, norm_gain, memory, *weights):
    rows, width = y_dec.shape
    tm_dev = memory.shape[0]
    return pl.pallas_call(
        first_kernel,
        out_shape=att_shapes(rows, width) + [jax.ShapeDtypeStruct((3, 2, tm_dev // 4, width), memory.dtype)],
        in_specs=[VMEM_SPEC] * 2 + [HBM_SPEC] * 5,
        out_specs=[VMEM_SPEC] * 3,
        scratch_shapes=[pltpu.VMEM((3, rows, width // 3), jnp.bfloat16)] + self_scratch(rows, width)
        + [pltpu.SemaphoreType.DMA] + [pltpu.SemaphoreType.DMA((3, 3))] * 2 + [CHUNK_SEMS] * 2
        + GATHER_SEMS,
        compiler_params=pltpu.CompilerParams(collective_id=0, has_side_effects=True,
                                             vmem_limit_bytes=24 * 1024 * 1024),
        name="first_layer",
    )(y_dec, norm_gain, in_hbm(memory.reshape(4, tm_dev // 4, width)), *map(in_hbm, weights))


def kv_kernel(info_ref, m_ref, wk_ref, wv_ref, k_ref, vt_ref):
    @pl.when(pl.program_id(0) < info_ref[3])
    def _():
        rows = m_ref[...]
        half = wk_ref.shape[2]
        both = matmul(rows, jnp.concatenate([wk_ref[0], wv_ref[0]], axis=1)).astype(jnp.bfloat16)
        k_ref[0] = both[:, :half]
        vt_ref[0] = jnp.transpose(both[:, half:])


def memory_kv(info, chip_memory, wk, wv):
    n_rows, width = chip_memory.shape
    half = width // 2
    layers = 1
    w_spec = pl.BlockSpec((layers, width, half), lambda t, info: (0, 0, info[1]))
    return pl.pallas_call(
        kv_kernel,
        grid_spec=pltpu.PrefetchScalarGridSpec(
            num_scalar_prefetch=1,
            grid=(n_rows // ROW_TILE,),
            in_specs=[pl.BlockSpec((ROW_TILE, width), lambda t, info: (t, 0)), w_spec, w_spec],
            out_specs=[pl.BlockSpec((layers, ROW_TILE, half), lambda t, info: (0, t, 0)),
                       pl.BlockSpec((layers, half, ROW_TILE), lambda t, info: (0, 0, t))],
        ),
        out_shape=[jax.ShapeDtypeStruct((layers, n_rows, half), jnp.bfloat16),
                   jax.ShapeDtypeStruct((layers, half, n_rows), jnp.bfloat16)],
        compiler_params=pltpu.CompilerParams(vmem_limit_bytes=24 * 1024 * 1024),
        name="memory_kv",
    )(info, chip_memory, in_hbm(wk), in_hbm(wv))


def spread_start(chip, from_z, from_core):
    return ((from_z * 16 + chip % 16) * 2 + from_core) * 4 * SPREAD_ROWS + chip // 16 * SPREAD_ROWS


def cross_kernel(info_ref, qt_ref, k_ref, vt_ref, out_ref, bias_ref, q0_ref, q1_ref, s0_ref, s1_ref):
    n_tiles = info_ref[3]
    n_q = q0_ref.shape[1]
    n_pairs = 3 * 4
    chip = info_ref[0]
    row = lax.broadcasted_iota(jnp.int32, (SPREAD_ROWS, LANES), 0)
    for block in range(bias_ref.shape[0] // SPREAD_ROWS):
        start = spread_start(chip, block // 2, block % 2)
        bias_ref[block * SPREAD_ROWS:(block + 1) * SPREAD_ROWS, :] = jnp.where(
            row < info_ref[2] - start, 0.0, NEG_BIG).astype(jnp.bfloat16)
    for ref in (q0_ref, q1_ref):
        lane_one = lax.broadcasted_iota(jnp.int32, (LANES, n_q), 0) == 0
        ref[LANES:256, :] = jnp.where(lane_one, 1.0, 0.0).astype(jnp.bfloat16)
        ref[0:LANES, :] = jnp.zeros((LANES, n_q), jnp.bfloat16)

    def set_query(ref, head, pair):
        part, tile = pair // 4, pair % 4
        rows = slice(head * HEAD, head * HEAD + HEAD)
        for i in range(4):
            ref[rows, i * LANES:i * LANES + LANES] = qt_ref[part, tile * 4 + i, rows, :]

    def rows_of(t):
        return pl.ds(pl.multiple_of(t * ROW_TILE, ROW_TILE), ROW_TILE)

    def fold(op, vals):
        return op(vals.reshape(ROW_TILE // 8, 8, n_q), axis=0)

    def score(t, q_ref, s_ref, pair, top):
        lanes = pl.ds(pl.multiple_of((pair // 4) * LANES, LANES), LANES)
        keys = jnp.concatenate([k_ref[rows_of(t), lanes], bias_ref[rows_of(t), :]], axis=1)
        s = matmul(keys, q_ref[...])
        s_ref[rows_of(t), :] = s
        return jnp.maximum(top, fold(jnp.max, s))

    def weigh(t, s_ref, pair, head, shift, total):
        w = jnp.exp2(s_ref[rows_of(t), :] * EXP_SCALE - shift)
        vals = pl.ds(pl.multiple_of((pair // 4) * LANES + head * HEAD, HEAD), HEAD)
        out_ref[pair // 4, pair % 4, head * HEAD:head * HEAD + HEAD, :] += matmul(
            vt_ref[vals, rows_of(t)], w.astype(jnp.bfloat16))
        return total + fold(jnp.sum, w)

    low_top = jnp.full((8, n_q), NEG_BIG, jnp.float32)
    no_sum = jnp.zeros((8, n_q), jnp.float32)

    def shift_of(top):
        return jnp.max(top, axis=0, keepdims=True) * EXP_SCALE

    def pair_step(pair, top0):
        part, tile = pair // 4, pair % 4
        out_ref[part, tile, 0:LANES, :] = jnp.zeros((LANES, n_q), jnp.float32)
        shift0 = shift_of(top0)
        set_query(q1_ref, 1, pair)

        def first(t, carry):
            top, total = carry
            return score(t, q1_ref, s1_ref, pair, top), weigh(t, s0_ref, pair, 0, shift0, total)

        top1, total0 = lax.fori_loop(0, n_tiles, first, (low_top, no_sum))
        shift1 = shift_of(top1)
        after = jnp.minimum(pair + 1, n_pairs - 1)
        set_query(q0_ref, 0, after)

        def second(t, carry):
            top, total = carry
            return score(t, q0_ref, s0_ref, after, top), weigh(t, s1_ref, pair, 1, shift1, total)

        next_top, total1 = lax.fori_loop(0, n_tiles, second, (low_top, no_sum))
        sums = [jnp.sum(v, axis=0, keepdims=True) for v in (total0, total1)]
        out_ref[part, tile, LANES:PART_ROWS, :] = jnp.concatenate([shift0, shift1] + sums + [shift0, shift1] + sums, axis=0)
        return next_top

    set_query(q0_ref, 0, 0)
    top0 = lax.fori_loop(0, n_tiles, lambda t, top: score(t, q0_ref, s0_ref, 0, top), low_top)
    lax.fori_loop(0, n_pairs, pair_step, top0)


def cross_attention(info, qt, keys, values):
    n_rows, half = keys.shape[1:]
    return pl.pallas_call(
        cross_kernel,
        grid_spec=pltpu.PrefetchScalarGridSpec(
            num_scalar_prefetch=1,
            grid=(1,),
            in_specs=[pl.BlockSpec(qt.shape, lambda i, info: (0, 0, 0, 0)),
                      pl.BlockSpec((None, n_rows, half), lambda i, info: (0, 0, 0)),
                      pl.BlockSpec((None, half, n_rows), lambda i, info: (0, 0, 0))],
            out_specs=pl.BlockSpec((3, 4, PART_ROWS, ROW_TILE), lambda i, info: (0, 0, 0, 0)),
            scratch_shapes=[pltpu.VMEM((n_rows, LANES), jnp.bfloat16)]
            + [pltpu.VMEM((256, ROW_TILE), jnp.bfloat16)] * 2 + [pltpu.VMEM((n_rows, ROW_TILE), jnp.float32)] * 2,
        ),
        out_shape=jax.ShapeDtypeStruct((3, 4, PART_ROWS, ROW_TILE), jnp.float32),
        compiler_params=pltpu.CompilerParams(vmem_limit_bytes=26 * 1024 * 1024),
        name="cross_attention",
    )(info, qt, keys, values)


def merge(pieces):
    tops = [p[LANES:130] for p in pieces]
    sums = [p[130:132] for p in pieces]
    top = functools.reduce(jnp.maximum, tops)
    fixes = [jnp.exp2(t - top) for t in tops]
    total = functools.reduce(jnp.add, [f * s for f, s in zip(fixes, sums)])
    outs = []
    for head in range(2):
        rows = slice(head * HEAD, head * HEAD + HEAD)
        outs.append(functools.reduce(jnp.add, [p[rows] * f[head:head + 1] for p, f in zip(pieces, fixes)]))
    return outs, top, total


def store_merged(ref, outs, top, total):
    ref[0:64] = outs[0]
    ref[64:LANES] = outs[1]
    ref[LANES:PART_ROWS] = jnp.concatenate([top, total, top, total], axis=0)


def finish_kernel(layer, last, part_ref, att_ref, hid_ref, gain_ref, w1_hbm, w3_hbm, w2_hbm, wo_hbm, co_hbm, *refs):
    if not last:
        next_weights, ck_hbm, cv_hbm, mem_ref = refs[:4], *refs[4:7]
        refs = refs[7:]
    n_out = 1 if last else 5
    outs_refs, refs = refs[:n_out], refs[n_out:]
    (w1, w3, w2, wo, co, recv1, acc1, recv2, acc2, recv3, turned, mine, full, x_ref,
     w_sem, cut_send, cut_recv, send_sem, recv_sem, sib_send, sib_recv) = refs[:21]
    pos, core = coords()
    loads = [pltpu.make_async_copy(src.at[layer], dst, w_sem.at[i]) for i, (src, dst) in enumerate(
        ((w1_hbm, w1), (w3_hbm, w3), (w2_hbm, w2), (wo_hbm, wo), (co_hbm, co)))]
    if not last:
        kv_ref, kv_sem, h_ref, w_ref, k_ref, v_ref, q_ref, nw_sem = refs[21:29]
        kv_loads = half_loads(layer + 1, core, (ck_hbm, cv_hbm), kv_ref, kv_sem)
        loads += kv_loads
        next_loads = half_loads(layer + 1, core, next_weights, w_ref, nw_sem)
        loads += next_loads
    for load in loads:
        load.start()
    entry_barrier(pos, core)

    def cut_lanes(part, cut):
        return pl.ds(pl.multiple_of((pos[ORDERS[part][1]] + cut) % 4 * LANES, LANES), LANES)

    def cut_copy(part, cut, dist):
        axis = ORDERS[part][0]
        peer = shifted(pos, axis, dist)
        return pltpu.make_async_remote_copy(
            src_ref=part_ref.at[part, peer[axis], :, cut_lanes(part, cut)], dst_ref=recv1.at[part, dist - 1, cut],
            send_sem=cut_send.at[part, cut, dist - 1], recv_sem=cut_recv.at[part, cut, dist - 1],
            device_id=device_of(peer, core), device_id_type=MESH)

    def copy(part, phase, dist):
        peer = shifted(pos, ORDERS[part][phase], dist)
        src, dst = ((acc1.at[part, dist], recv2.at[part, dist - 1]), (acc2.at[part], recv3.at[part, dist - 1]))[phase - 1]
        return pltpu.make_async_remote_copy(
            src_ref=src, dst_ref=dst, send_sem=send_sem.at[part, phase, dist - 1],
            recv_sem=recv_sem.at[part, phase, dist - 1], device_id=device_of(peer, core), device_id_type=MESH)

    copies = {}
    cuts = FAR_FIRST + (0,)
    for cut in cuts:
        for dist in FAR_FIRST:
            for part in PARTS:
                copies[part, 0, cut, dist] = cut_copy(part, cut, dist)
                copies[part, 0, cut, dist].start()

    hidden = hid_ref[...]
    normed = rms_norm(hidden, gain_ref[layer:layer + 1, :])
    for load in loads[:3]:
        load.wait()
    activated = (jax.nn.silu(matmul(normed, w1[...])) * matmul(normed, w3[...])).astype(jnp.bfloat16)
    mlp_part = matmul(activated, w2[...])

    if not last:
        for load in kv_loads:
            load.wait()

        def kv_tile(t, carry):
            at = pl.ds(pl.multiple_of(t * ROW_TILE, ROW_TILE), ROW_TILE)
            made = matmul(mem_ref[at, :], kv_ref[...]).astype(jnp.bfloat16)
            half = made.shape[1] // 2
            outs_refs[3][0, at, :] = made[:, :half]
            outs_refs[4][0, :, at] = jnp.transpose(made[:, half:])
            return carry

        lax.fori_loop(0, mem_ref.shape[0] // ROW_TILE, kv_tile, 0)

    for cut in cuts:
        for part in PARTS:
            for dist in NEAR_FIRST:
                copies[part, 0, cut, dist].wait_recv()
            own = pos[ORDERS[part][0]]
            mine_cut = part_ref[part, own, :, cut_lanes(part, cut)]
            store_merged(acc1.at[part, cut], *merge([mine_cut] + [recv1[part, d, cut] for d in PARTS]))
            if cut:
                copies[part, 1, cut] = copy(part, 1, cut)
                copies[part, 1, cut].start()
    for part in PARTS:
        for dist in NEAR_FIRST:
            copies[part, 1, dist].wait_recv()
        store_merged(acc2.at[part], *merge([acc1[part, 0]] + [recv2[part, d] for d in PARTS]))
        for dist in FAR_FIRST:
            copies[part, 2, dist] = copy(part, 2, dist)
            copies[part, 2, dist].start()
    mine[0] = att_ref[...]
    for part in PARTS:
        for dist in NEAR_FIRST:
            copies[part, 2, dist].wait_recv()
        outs, top, total = merge([acc2[part]] + [recv3[part, d] for d in PARTS])
        turned[part] = jnp.transpose(jnp.concatenate([outs[h] / total[h:h + 1] for h in range(2)], axis=0))
        rows = pl.ds(pl.multiple_of(pos[ORDERS[part][2]] * 32, 32), 32)
        mine[1, :, part * LANES:part * LANES + LANES] = turned[part, rows, :].astype(jnp.bfloat16)
    n_own = hid_ref.shape[0]
    theirs = pl.ds(pl.multiple_of((1 - core) * n_own, n_own), n_own)
    last_copy = pltpu.make_async_remote_copy(
        src_ref=mine.at[:, theirs], dst_ref=full.at[core], send_sem=sib_send, recv_sem=sib_recv,
        device_id=device_of(pos, 1 - core), device_id_type=MESH)
    last_copy.start()
    own_rows = pl.ds(pl.multiple_of(core * n_own, n_own), n_own)
    full[core] = mine[:, own_rows]
    for load in loads[3:5]:
        load.wait()
    last_copy.wait()
    parts = []
    for i, weight in enumerate((wo, co)):
        parts.append(matmul(jnp.concatenate([full[0, i], full[1, i]], axis=1), weight[...]))
    result = (hidden.astype(jnp.float32) + parts[0] + parts[1] + mlp_part).astype(jnp.bfloat16)
    outs_refs[0][...] = result
    if not last:
        store_normed(x_ref, result, gain_ref[layer + 1:layer + 2, :])
        run_gather(x_ref, h_ref, refs[29:], pos, core)
        for load in next_loads:
            load.wait()
        self_body(pos, h_ref, w_ref, k_ref, v_ref, q_ref, outs_refs[1], outs_refs[2])
    for one in copies.values():
        one.wait_send()


def finish_layer(layer, last, partial, att, hidden, gain, w1, w3, w2, wo, co, next_weights=(), memory=None):
    f32, bf16 = jnp.float32, jnp.bfloat16
    n_rows, half = att.shape
    rows, width = hidden.shape
    ff = w1.shape[2]
    third = width // 3
    out_shape = [jax.ShapeDtypeStruct(hidden.shape, bf16)]
    if not last:
        out_shape += att_shapes(rows, width)
        out_shape += [jax.ShapeDtypeStruct((1, memory.shape[0], half), bf16),
                      jax.ShapeDtypeStruct((1, half, memory.shape[0]), bf16)]
    return pl.pallas_call(
        functools.partial(finish_kernel, layer, last),
        out_shape=out_shape,
        in_specs=[VMEM_SPEC] * 4 + [HBM_SPEC] * (5 + len(next_weights)) + ([] if last else [VMEM_SPEC]),
        out_specs=[VMEM_SPEC] * len(out_shape),
        scratch_shapes=[pltpu.VMEM((width, ff), bf16), pltpu.VMEM((width, ff), bf16), pltpu.VMEM((ff, width), bf16),
                        pltpu.VMEM((width, width), bf16), pltpu.VMEM((width, width), bf16),
                        pltpu.VMEM((3, 3, 4, PART_ROWS, LANES), f32), pltpu.VMEM((3, 4, PART_ROWS, LANES), f32),
                        pltpu.VMEM((3, 3, PART_ROWS, LANES), f32), pltpu.VMEM((3, PART_ROWS, LANES), f32),
                        pltpu.VMEM((3, 3, PART_ROWS, LANES), f32), pltpu.VMEM((3, LANES, LANES), f32),
                        pltpu.VMEM((2, n_rows, half), bf16), pltpu.VMEM((2, 2, rows, half), bf16),
                        pltpu.VMEM((3, rows, third), bf16),
                        pltpu.SemaphoreType.DMA((5,)), CUT_SEMS, CUT_SEMS,
                        PHASE_SEMS, PHASE_SEMS,
                        pltpu.SemaphoreType.DMA, pltpu.SemaphoreType.DMA]
        + ([] if last else [pltpu.VMEM((width, width), bf16), pltpu.SemaphoreType.DMA((2,))]
           + self_scratch(rows, width) + GATHER_SEMS),
        compiler_params=pltpu.CompilerParams(collective_id=1 + layer, has_side_effects=True,
                                             vmem_limit_bytes=36 * 1024 * 1024),
        name="finish_layer",
    )(partial, att, hidden, gain, *map(in_hbm, (w1, w3, w2, wo, co) + next_weights), *([] if last else [memory]))


def solution(mesh):
    row_spec = P(("dp", "sp"), None)
    full_spec = P()

    def device_step(y_dec, memory, mem_len, norm_gain, self_wq, self_wk, self_wv, self_wo, cross_wq, cross_wk, cross_wv, cross_wo, mlp_gate, mlp_up, mlp_down):
        tq_dev, width = y_dec.shape
        tm_dev = memory.shape[0]
        sp = lax.axis_index("sp")
        chip = sp // 2
        tiles = [jnp.where(spread_start(chip, z, 0) < mem_len[0], 1, 0) for z in PARTS]
        info = jnp.stack([chip, sp % 2, mem_len[0], sum(tiles)]).astype(jnp.int32)
        weights = (self_wk, self_wv, cross_wq, self_wq)
        att, qt, rows = first_layer(y_dec, norm_gain, memory, *weights)
        rows = rows.reshape(3 * tm_dev // 2, width)
        keys, values = memory_kv(info, rows, cross_wk, cross_wv)
        hidden = y_dec
        layers = norm_gain.shape[0]
        for layer in range(layers):
            partial = cross_attention(info, qt, keys, values)
            last = layer == layers - 1
            out = finish_layer(layer, last, partial, att, hidden, norm_gain, mlp_gate, mlp_up, mlp_down, self_wo,
                               cross_wo, *(() if last else (weights + (cross_wk, cross_wv), rows)))
            hidden = out[0]
            if not last:
                att, qt, keys, values = out[1:]
        return hidden

    return jax.shard_map(device_step, mesh=mesh, in_specs=(row_spec, row_spec, P("dp")) + (full_spec,) * 12, out_specs=row_spec, check_vma=False)
```

```python
import functools
import math

import jax
import jax.numpy as jnp
from jax import lax
from jax.experimental import pallas as pl
from jax.experimental.pallas import tpu as pltpu
from jax.sharding import PartitionSpec as P

HEAD = 64
NORM_EPS = 1e-6
NEG_BIG = -1e30
MESH = pl.DeviceIdType.MESH
EXP_SCALE = HEAD ** -0.5 * math.log2(math.e)
ORDERS = ((0, 1, 2), (1, 2, 0), (2, 0, 1))
VMEM_SPEC = pl.BlockSpec(memory_space=pltpu.VMEM)
ROW_TILE = 512
LANES = 128
PART_ROWS = 136
PARTS = range(3)
NEAR_FIRST = (1, 3, 2)
FAR_FIRST = (2, 1, 3)
PHASE_SEMS = pltpu.SemaphoreType.DMA((3, 3, 3))
CUT_SEMS = pltpu.SemaphoreType.DMA((3, 4, 3))
CHUNK_SEMS = pltpu.SemaphoreType.DMA((3, 4))


def in_hbm(array):
    return pltpu.with_memory_space_constraint(array, pltpu.HBM)


def matmul(left_mat, right_mat):
    return jnp.dot(left_mat, right_mat, preferred_element_type=jnp.float32)


def rms_norm(hidden, gain_vec):
    wide_vals = hidden.astype(jnp.float32)
    inv_rms = lax.rsqrt(jnp.mean(wide_vals * wide_vals, axis=-1, keepdims=True) + NORM_EPS)
    return (wide_vals * inv_rms * gain_vec.astype(jnp.float32)).astype(jnp.bfloat16)


def coords():
    sp = lax.axis_index("sp")
    return (sp // 32, (sp // 8) % 4, (sp // 2) % 4), sp % 2


def device_of(pos, core):
    return {"sp": ((pos[0] * 4 + pos[1]) * 4 + pos[2]) * 2 + core}


def shifted(pos, axis, dist):
    return tuple((c + dist) % 4 if i == axis else c for i, c in enumerate(pos))


def entry_barrier(pos, core):
    sem = pltpu.get_barrier_semaphore()
    for axis in PARTS:
        for dist in NEAR_FIRST:
            pl.semaphore_signal(sem, inc=1, device_id=device_of(shifted(pos, axis, dist), core), device_id_type=MESH)
    pl.semaphore_signal(sem, inc=1, device_id=device_of(pos, 1 - core), device_id_type=MESH)
    pl.semaphore_wait(sem, 10)


def gather_slice(ref, part, free, pos, core):
    idx = [part] + [slice(None) if axis in free else pos[axis] for axis in PARTS]
    return ref.at[tuple(idx) + (core,)]


GATHER_SEMS = [pltpu.SemaphoreType.DMA((3,)), PHASE_SEMS, PHASE_SEMS,
               CHUNK_SEMS, CHUNK_SEMS,
               CUT_SEMS, CUT_SEMS]


def run_gather(x_ref, out_ref, sems, pos, core, after_phase=None):
    local_sem, send_sem, recv_sem, sib_send, sib_recv, last_send, last_recv = sems
    sibling = device_of(pos, 1 - core)

    def phase_copy(part, phase, dist):
        order = ORDERS[part]
        dst = gather_slice(out_ref, part, order[:phase], pos, core)
        return pltpu.make_async_remote_copy(
            src_ref=x_ref.at[part] if phase == 0 else dst, dst_ref=dst, send_sem=send_sem.at[part, phase, dist - 1],
            recv_sem=recv_sem.at[part, phase, dist - 1],
            device_id=device_of(shifted(pos, order[phase], dist), core), device_id_type=MESH)

    def sibling_copy(part, dist):
        order = ORDERS[part]
        ref = gather_slice(out_ref, part, order[:2], shifted(pos, order[2], 4 - dist), core)
        return pltpu.make_async_remote_copy(
            src_ref=ref, dst_ref=ref, send_sem=sib_send.at[part, dist], recv_sem=sib_recv.at[part, dist],
            device_id=sibling, device_id_type=MESH)

    local = [pltpu.make_async_copy(x_ref.at[p], gather_slice(out_ref, p, (), pos, core), local_sem.at[p])
             for p in PARTS]
    def last_copy(part, near, dist):
        order = ORDERS[part]
        ref = gather_slice(out_ref, part, order[:1], shifted(pos, order[1], 4 - near), core)
        return pltpu.make_async_remote_copy(
            src_ref=ref, dst_ref=ref, send_sem=last_send.at[part, near, dist - 1],
            recv_sem=last_recv.at[part, near, dist - 1],
            device_id=device_of(shifted(pos, order[2], dist), core), device_id_type=MESH)

    copies = {}

    def begin(key, copy):
        copies[key] = copy
        copy.start()

    def send_last(part, near):
        for dist in FAR_FIRST:
            begin((part, 2, near, dist), last_copy(part, near, dist))

    def after(phase):
        if after_phase is not None:
            after_phase(phase)

    for part in PARTS:
        for dist in FAR_FIRST:
            begin((part, 0, dist), phase_copy(part, 0, dist))
        local[part].start()
    after(0)
    for part in PARTS:
        local[part].wait()
        for dist in NEAR_FIRST:
            copies[part, 0, dist].wait_recv()
        for dist in FAR_FIRST:
            begin((part, 1, dist), phase_copy(part, 1, dist))
    for part in PARTS:
        send_last(part, 0)
    after(1)
    for near in NEAR_FIRST:
        for part in PARTS:
            copies[part, 1, near].wait_recv()
            send_last(part, near)
    for part in PARTS:
        begin((part, 3, 0), sibling_copy(part, 0))
    after(2)
    for dist in NEAR_FIRST:
        for part in PARTS:
            for near in range(4):
                copies[part, 2, near, dist].wait_recv()
            begin((part, 3, dist), sibling_copy(part, dist))
    for part in PARTS:
        for dist in range(4):
            copies[part, 3, dist].wait_recv()
    for copy in copies.values():
        copy.wait_send()


def store_normed(x_ref, hidden, gain_vec):
    normed = rms_norm(hidden, gain_vec)
    third = x_ref.shape[2]
    for part in PARTS:
        x_ref[part] = normed[:, part * third:part * third + third]


def self_scratch(rows, width):
    bf16 = jnp.bfloat16
    half = width // 2
    n_rows = LANES * rows
    return [pltpu.VMEM((3, 4, 4, 4, 2, rows, width // 3), bf16), pltpu.VMEM((width, 4 * half), bf16),
            pltpu.VMEM((n_rows, half), bf16), pltpu.VMEM((n_rows, half), bf16),
            pltpu.VMEM((4, 4, 4, 2 * rows, half), bf16), pltpu.SemaphoreType.DMA((4,))]


def half_loads(layer, core, weights, w_ref, w_sem):
    half = w_ref.shape[1] // len(weights)
    cols = pl.ds(pl.multiple_of(core * half, half), half)
    return [pltpu.make_async_copy(weight.at[layer, :, cols], w_ref.at[:, i * half:i * half + half], w_sem.at[i])
            for i, weight in enumerate(weights)]


def self_body(pos, h_ref, w_ref, k_ref, v_ref, q_ref, att_ref, qt_ref):
    half = k_ref.shape[1]
    n_query = att_ref.shape[0]
    chip = (pos[0] * 4 + pos[1]) * 4 + pos[2]

    def rows_cat(z, y, x):
        return jnp.concatenate([h_ref[p, z, y, x].reshape(n_query, -1) for p in PARTS], axis=1)

    def key_tile(z, carry):
        rows = jnp.concatenate([rows_cat(z, y, x) for y in range(4) for x in range(4)], axis=0)
        at = pl.ds(pl.multiple_of(z * ROW_TILE, ROW_TILE), ROW_TILE)
        made = matmul(rows, w_ref[:, :3 * half]).astype(jnp.bfloat16)
        k_ref[at, :] = made[:, :half]
        v_ref[at, :] = made[:, half:2 * half]
        q_ref[z] = made[:, 2 * half:].reshape(4, 4, n_query, half)
        return carry

    lax.fori_loop(0, 4, key_tile, 0)

    for part in PARTS:
        cols = slice(part * LANES, part * LANES + LANES)

        def query_tile(a, carry, part=part, cols=cols):
            order = ORDERS[part]
            for b in range(4):
                blocks = []
                for c in range(4):
                    at = [None] * 3
                    at[order[0]], at[order[1]], at[order[2]] = a, b, c
                    blocks.append(q_ref[at[0], at[1], at[2], :, cols])
                qt_ref[part, a * 4 + b] = jnp.transpose(jnp.concatenate(blocks, axis=0))
            return carry

        lax.fori_loop(0, 4, query_tile, 0)

    query = matmul(rows_cat(*pos), w_ref[:, 3 * half:]).astype(jnp.bfloat16)
    n_keys = k_ref.shape[0]
    low = lax.broadcasted_iota(jnp.int32, (n_query, LANES), 1) < HEAD
    key_pos = lax.broadcasted_iota(jnp.int32, (2 * n_query, n_keys), 1)
    query_pos = chip * n_query + lax.broadcasted_iota(jnp.int32, (2 * n_query, n_keys), 0) % n_query
    causal = key_pos <= query_pos
    zero = jnp.zeros((n_query, LANES), jnp.bfloat16)
    for part in PARTS:
        cols = slice(part * LANES, part * LANES + LANES)
        q_pair = query[:, cols]
        q_two = jnp.concatenate([jnp.where(low, q_pair, zero), jnp.where(low, zero, q_pair)], axis=0)
        s = lax.dot_general(q_two, k_ref[:, cols], (((1,), (1,)), ((), ())), preferred_element_type=jnp.float32)
        s = jnp.where(causal, s, NEG_BIG)
        top = jnp.max(s, axis=1, keepdims=True)
        w = jnp.exp2((s - top) * EXP_SCALE)
        total = jnp.sum(w, axis=1, keepdims=True)
        o = matmul(w.astype(jnp.bfloat16), v_ref[:, cols]) / total
        att_ref[:, cols] = jnp.where(low, o[:n_query], o[n_query:]).astype(jnp.bfloat16)


SPREAD = ((0, 64), (64, 64), (LANES, LANES))
SPREAD_ROWS = 256


def first_kernel(y_ref, gain_ref, mem_ref, wk, wv, cq, wq, att_ref, qt_ref, mem_out,
                 x_ref, h_ref, w_ref, k_ref, v_ref, q_ref, w_sem,
                 local_sem, ex_send, ex_recv, fw_send, fw_recv, *sems):
    pos, core = coords()
    loads = half_loads(0, core, (wk, wv, cq, wq), w_ref, w_sem)
    for load in loads:
        load.start()
    z = pos[0]
    own = pltpu.make_async_copy(mem_ref.at[jnp.minimum(z, 2)], mem_out.at[jnp.minimum(z, 2), core], local_sem)
    entry_barrier(pos, core)
    sibling = device_of(pos, 1 - core)

    def spread_copy(dist, piece):
        to = (z + dist) % 4
        start, size = SPREAD[piece]
        rows = pl.ds(start, size)
        return pltpu.make_async_remote_copy(
            src_ref=mem_ref.at[to, rows], dst_ref=mem_out.at[jnp.minimum(z, 2), core, rows],
            send_sem=ex_send.at[piece, dist - 1], recv_sem=ex_recv.at[piece, dist - 1],
            device_id=device_of(shifted(pos, 0, dist), core), device_id_type=MESH)

    def forward_copy(dist, piece):
        at = jnp.minimum((z + 4 - dist) % 4, 2)
        start, size = SPREAD[piece]
        rows = pl.ds(start, size)
        src = mem_ref.at[at, rows] if dist == 0 else mem_out.at[at, core, rows]
        return pltpu.make_async_remote_copy(
            src_ref=src, dst_ref=mem_out.at[at, core, rows], send_sem=fw_send.at[piece, dist],
            recv_sem=fw_recv.at[piece, dist], device_id=sibling, device_id_type=MESH)

    def spread(piece):
        @pl.when(z < 3)
        def _():
            for dist in FAR_FIRST:
                spread_copy(dist, piece).start()

    def forward(piece):
        @pl.when(z < 3)
        def _():
            forward_copy(0, piece).start()
        for dist in NEAR_FIRST:
            @pl.when((z + 4 - dist) % 4 < 3)
            def _(dist=dist):
                spread_copy(dist, piece).wait_recv()
                forward_copy(dist, piece).start()

    @pl.when(z < 3)
    def _():
        own.start()
    store_normed(x_ref, y_ref[...], gain_ref[0:1, :])
    run_gather(x_ref, h_ref, sems, pos, core, after_phase=spread)
    for load in loads:
        load.wait()
    for piece in range(2):
        forward(piece)
    self_body(pos, h_ref, w_ref, k_ref, v_ref, q_ref, att_ref, qt_ref)
    forward(2)

    @pl.when(z < 3)
    def _():
        own.wait()
        for piece in PARTS:
            for dist in NEAR_FIRST:
                spread_copy(dist, piece).wait_send()
    for piece in PARTS:
        for dist in range(4):
            @pl.when((z + 4 - dist) % 4 < 3)
            def _(dist=dist, piece=piece):
                forward_copy(dist, piece).wait()


def att_shapes(rows, width):
    return [jax.ShapeDtypeStruct((2 * rows, width // 2), jnp.bfloat16),
            jax.ShapeDtypeStruct((3, 16, LANES, LANES), jnp.bfloat16)]


HBM_SPEC = pl.BlockSpec(memory_space=pltpu.HBM)


def first_layer(y_dec, norm_gain, memory, *weights):
    rows, width = y_dec.shape
    tm_dev = memory.shape[0]
    return pl.pallas_call(
        first_kernel,
        out_shape=att_shapes(rows, width) + [jax.ShapeDtypeStruct((3, 2, tm_dev // 4, width), memory.dtype)],
        in_specs=[VMEM_SPEC] * 2 + [HBM_SPEC] * 5,
        out_specs=[VMEM_SPEC] * 3,
        scratch_shapes=[pltpu.VMEM((3, rows, width // 3), jnp.bfloat16)] + self_scratch(rows, width)
        + [pltpu.SemaphoreType.DMA] + [pltpu.SemaphoreType.DMA((3, 3))] * 2 + [CHUNK_SEMS] * 2
        + GATHER_SEMS,
        compiler_params=pltpu.CompilerParams(collective_id=0, has_side_effects=True,
                                             vmem_limit_bytes=24 * 1024 * 1024),
        name="first_layer",
    )(y_dec, norm_gain, in_hbm(memory.reshape(4, tm_dev // 4, width)), *map(in_hbm, weights))


def kv_kernel(info_ref, m_ref, wk_ref, wv_ref, k_ref, vt_ref):
    @pl.when(pl.program_id(0) < info_ref[3])
    def _():
        rows = m_ref[...]
        half = wk_ref.shape[2]
        both = matmul(rows, jnp.concatenate([wk_ref[0], wv_ref[0]], axis=1)).astype(jnp.bfloat16)
        k_ref[0] = both[:, :half]
        vt_ref[0] = jnp.transpose(both[:, half:])


def memory_kv(info, chip_memory, wk, wv):
    n_rows, width = chip_memory.shape
    half = width // 2
    layers = 1
    w_spec = pl.BlockSpec((layers, width, half), lambda t, info: (0, 0, info[1]))
    return pl.pallas_call(
        kv_kernel,
        grid_spec=pltpu.PrefetchScalarGridSpec(
            num_scalar_prefetch=1,
            grid=(n_rows // ROW_TILE,),
            in_specs=[pl.BlockSpec((ROW_TILE, width), lambda t, info: (t, 0)), w_spec, w_spec],
            out_specs=[pl.BlockSpec((layers, ROW_TILE, half), lambda t, info: (0, t, 0)),
                       pl.BlockSpec((layers, half, ROW_TILE), lambda t, info: (0, 0, t))],
        ),
        out_shape=[jax.ShapeDtypeStruct((layers, n_rows, half), jnp.bfloat16),
                   jax.ShapeDtypeStruct((layers, half, n_rows), jnp.bfloat16)],
        compiler_params=pltpu.CompilerParams(vmem_limit_bytes=24 * 1024 * 1024),
        name="memory_kv",
    )(info, chip_memory, in_hbm(wk), in_hbm(wv))


def spread_start(chip, from_z, from_core):
    return ((from_z * 16 + chip % 16) * 2 + from_core) * 4 * SPREAD_ROWS + chip // 16 * SPREAD_ROWS


def cross_kernel(info_ref, qt_ref, k_ref, vt_ref, out_ref, bias_ref, q0_ref, q1_ref, s0_ref, s1_ref):
    n_tiles = info_ref[3]
    n_q = q0_ref.shape[1]
    n_pairs = 3 * 4
    chip = info_ref[0]
    row = lax.broadcasted_iota(jnp.int32, (SPREAD_ROWS, LANES), 0)
    for block in range(bias_ref.shape[0] // SPREAD_ROWS):
        start = spread_start(chip, block // 2, block % 2)
        bias_ref[block * SPREAD_ROWS:(block + 1) * SPREAD_ROWS, :] = jnp.where(
            row < info_ref[2] - start, 0.0, NEG_BIG).astype(jnp.bfloat16)
    for ref in (q0_ref, q1_ref):
        lane_one = lax.broadcasted_iota(jnp.int32, (LANES, n_q), 0) == 0
        ref[LANES:256, :] = jnp.where(lane_one, 1.0, 0.0).astype(jnp.bfloat16)
        ref[0:LANES, :] = jnp.zeros((LANES, n_q), jnp.bfloat16)

    def set_query(ref, head, pair):
        part, tile = pair // 4, pair % 4
        rows = slice(head * HEAD, head * HEAD + HEAD)
        for i in range(4):
            ref[rows, i * LANES:i * LANES + LANES] = qt_ref[part, tile * 4 + i, rows, :]

    def rows_of(t):
        return pl.ds(pl.multiple_of(t * ROW_TILE, ROW_TILE), ROW_TILE)

    def fold(op, vals):
        return op(vals.reshape(ROW_TILE // 8, 8, n_q), axis=0)

    def score(t, q_ref, s_ref, pair, top):
        lanes = pl.ds(pl.multiple_of((pair // 4) * LANES, LANES), LANES)
        keys = jnp.concatenate([k_ref[rows_of(t), lanes], bias_ref[rows_of(t), :]], axis=1)
        s = matmul(keys, q_ref[...])
        s_ref[rows_of(t), :] = s
        return jnp.maximum(top, fold(jnp.max, s))

    def weigh(t, s_ref, pair, head, shift, total):
        w = jnp.exp2(s_ref[rows_of(t), :] * EXP_SCALE - shift)
        vals = pl.ds(pl.multiple_of((pair // 4) * LANES + head * HEAD, HEAD), HEAD)
        out_ref[pair // 4, pair % 4, head * HEAD:head * HEAD + HEAD, :] += matmul(
            vt_ref[vals, rows_of(t)], w.astype(jnp.bfloat16))
        return total + fold(jnp.sum, w)

    low_top = jnp.full((8, n_q), NEG_BIG, jnp.float32)
    no_sum = jnp.zeros((8, n_q), jnp.float32)

    def shift_of(top):
        return jnp.max(top, axis=0, keepdims=True) * EXP_SCALE

    def pair_step(pair, top0):
        part, tile = pair // 4, pair % 4
        out_ref[part, tile, 0:LANES, :] = jnp.zeros((LANES, n_q), jnp.float32)
        shift0 = shift_of(top0)
        set_query(q1_ref, 1, pair)

        def first(t, carry):
            top, total = carry
            return score(t, q1_ref, s1_ref, pair, top), weigh(t, s0_ref, pair, 0, shift0, total)

        top1, total0 = lax.fori_loop(0, n_tiles, first, (low_top, no_sum))
        shift1 = shift_of(top1)
        after = jnp.minimum(pair + 1, n_pairs - 1)
        set_query(q0_ref, 0, after)

        def second(t, carry):
            top, total = carry
            return score(t, q0_ref, s0_ref, after, top), weigh(t, s1_ref, pair, 1, shift1, total)

        next_top, total1 = lax.fori_loop(0, n_tiles, second, (low_top, no_sum))
        sums = [jnp.sum(v, axis=0, keepdims=True) for v in (total0, total1)]
        out_ref[part, tile, LANES:PART_ROWS, :] = jnp.concatenate([shift0, shift1] + sums + [shift0, shift1] + sums, axis=0)
        return next_top

    set_query(q0_ref, 0, 0)
    top0 = lax.fori_loop(0, n_tiles, lambda t, top: score(t, q0_ref, s0_ref, 0, top), low_top)
    lax.fori_loop(0, n_pairs, pair_step, top0)


def cross_attention(info, qt, keys, values):
    n_rows, half = keys.shape[1:]
    return pl.pallas_call(
        cross_kernel,
        grid_spec=pltpu.PrefetchScalarGridSpec(
            num_scalar_prefetch=1,
            grid=(1,),
            in_specs=[pl.BlockSpec(qt.shape, lambda i, info: (0, 0, 0, 0)),
                      pl.BlockSpec((None, n_rows, half), lambda i, info: (0, 0, 0)),
                      pl.BlockSpec((None, half, n_rows), lambda i, info: (0, 0, 0))],
            out_specs=pl.BlockSpec((3, 4, PART_ROWS, ROW_TILE), lambda i, info: (0, 0, 0, 0)),
            scratch_shapes=[pltpu.VMEM((n_rows, LANES), jnp.bfloat16)]
            + [pltpu.VMEM((256, ROW_TILE), jnp.bfloat16)] * 2 + [pltpu.VMEM((n_rows, ROW_TILE), jnp.float32)] * 2,
        ),
        out_shape=jax.ShapeDtypeStruct((3, 4, PART_ROWS, ROW_TILE), jnp.float32),
        compiler_params=pltpu.CompilerParams(vmem_limit_bytes=26 * 1024 * 1024),
        name="cross_attention",
    )(info, qt, keys, values)


def merge(pieces):
    tops = [p[LANES:130] for p in pieces]
    sums = [p[130:132] for p in pieces]
    top = functools.reduce(jnp.maximum, tops)
    fixes = [jnp.exp2(t - top) for t in tops]
    total = functools.reduce(jnp.add, [f * s for f, s in zip(fixes, sums)])
    outs = []
    for head in range(2):
        rows = slice(head * HEAD, head * HEAD + HEAD)
        outs.append(functools.reduce(jnp.add, [p[rows] * f[head:head + 1] for p, f in zip(pieces, fixes)]))
    return outs, top, total


def store_merged(ref, outs, top, total):
    ref[0:64] = outs[0]
    ref[64:LANES] = outs[1]
    ref[LANES:PART_ROWS] = jnp.concatenate([top, total, top, total], axis=0)


def finish_kernel(layer, last, part_ref, att_ref, hid_ref, gain_ref, w1_hbm, w3_hbm, w2_hbm, wo_hbm, co_hbm, *refs):
    if not last:
        next_weights, ck_hbm, cv_hbm, mem_ref = refs[:4], *refs[4:7]
        refs = refs[7:]
    n_out = 1 if last else 5
    outs_refs, refs = refs[:n_out], refs[n_out:]
    (w1, w3, w2, wo, co, recv1, acc1, recv2, acc2, recv3, turned, mine, full, x_ref,
     w_sem, cut_send, cut_recv, send_sem, recv_sem, sib_send, sib_recv) = refs[:21]
    pos, core = coords()
    loads = [pltpu.make_async_copy(src.at[layer], dst, w_sem.at[i]) for i, (src, dst) in enumerate(
        ((w1_hbm, w1), (w3_hbm, w3), (w2_hbm, w2), (wo_hbm, wo), (co_hbm, co)))]
    if not last:
        kv_ref, kv_sem, h_ref, w_ref, k_ref, v_ref, q_ref, nw_sem = refs[21:29]
        kv_loads = half_loads(layer + 1, core, (ck_hbm, cv_hbm), kv_ref, kv_sem)
        loads += kv_loads
        next_loads = half_loads(layer + 1, core, next_weights, w_ref, nw_sem)
        loads += next_loads
    for load in loads:
        load.start()
    entry_barrier(pos, core)

    def cut_lanes(part, cut):
        return pl.ds(pl.multiple_of((pos[ORDERS[part][1]] + cut) % 4 * LANES, LANES), LANES)

    def cut_copy(part, cut, dist):
        axis = ORDERS[part][0]
        peer = shifted(pos, axis, dist)
        return pltpu.make_async_remote_copy(
            src_ref=part_ref.at[part, peer[axis], :, cut_lanes(part, cut)], dst_ref=recv1.at[part, dist - 1, cut],
            send_sem=cut_send.at[part, cut, dist - 1], recv_sem=cut_recv.at[part, cut, dist - 1],
            device_id=device_of(peer, core), device_id_type=MESH)

    def copy(part, phase, dist):
        peer = shifted(pos, ORDERS[part][phase], dist)
        src, dst = ((acc1.at[part, dist], recv2.at[part, dist - 1]), (acc2.at[part], recv3.at[part, dist - 1]))[phase - 1]
        return pltpu.make_async_remote_copy(
            src_ref=src, dst_ref=dst, send_sem=send_sem.at[part, phase, dist - 1],
            recv_sem=recv_sem.at[part, phase, dist - 1], device_id=device_of(peer, core), device_id_type=MESH)

    copies = {}
    cuts = FAR_FIRST + (0,)
    for cut in cuts:
        for dist in FAR_FIRST:
            for part in PARTS:
                copies[part, 0, cut, dist] = cut_copy(part, cut, dist)
                copies[part, 0, cut, dist].start()

    hidden = hid_ref[...]
    normed = rms_norm(hidden, gain_ref[layer:layer + 1, :])
    for load in loads[:3]:
        load.wait()
    activated = (jax.nn.silu(matmul(normed, w1[...])) * matmul(normed, w3[...])).astype(jnp.bfloat16)
    mlp_part = matmul(activated, w2[...])

    if not last:
        for load in kv_loads:
            load.wait()

        def kv_tile(t, carry):
            at = pl.ds(pl.multiple_of(t * ROW_TILE, ROW_TILE), ROW_TILE)
            made = matmul(mem_ref[at, :], kv_ref[...]).astype(jnp.bfloat16)
            half = made.shape[1] // 2
            outs_refs[3][0, at, :] = made[:, :half]
            outs_refs[4][0, :, at] = jnp.transpose(made[:, half:])
            return carry

        lax.fori_loop(0, mem_ref.shape[0] // ROW_TILE, kv_tile, 0)

    for cut in cuts:
        for part in PARTS:
            for dist in NEAR_FIRST:
                copies[part, 0, cut, dist].wait_recv()
            own = pos[ORDERS[part][0]]
            mine_cut = part_ref[part, own, :, cut_lanes(part, cut)]
            store_merged(acc1.at[part, cut], *merge([mine_cut] + [recv1[part, d, cut] for d in PARTS]))
            if cut:
                copies[part, 1, cut] = copy(part, 1, cut)
                copies[part, 1, cut].start()
    for part in PARTS:
        for dist in NEAR_FIRST:
            copies[part, 1, dist].wait_recv()
        store_merged(acc2.at[part], *merge([acc1[part, 0]] + [recv2[part, d] for d in PARTS]))
        for dist in FAR_FIRST:
            copies[part, 2, dist] = copy(part, 2, dist)
            copies[part, 2, dist].start()
    mine[0] = att_ref[...]
    for part in PARTS:
        for dist in NEAR_FIRST:
            copies[part, 2, dist].wait_recv()
        outs, top, total = merge([acc2[part]] + [recv3[part, d] for d in PARTS])
        turned[part] = jnp.transpose(jnp.concatenate([outs[h] / total[h:h + 1] for h in range(2)], axis=0))
        rows = pl.ds(pl.multiple_of(pos[ORDERS[part][2]] * 32, 32), 32)
        mine[1, :, part * LANES:part * LANES + LANES] = turned[part, rows, :].astype(jnp.bfloat16)
    n_own = hid_ref.shape[0]
    theirs = pl.ds(pl.multiple_of((1 - core) * n_own, n_own), n_own)
    last_copy = pltpu.make_async_remote_copy(
        src_ref=mine.at[:, theirs], dst_ref=full.at[core], send_sem=sib_send, recv_sem=sib_recv,
        device_id=device_of(pos, 1 - core), device_id_type=MESH)
    last_copy.start()
    own_rows = pl.ds(pl.multiple_of(core * n_own, n_own), n_own)
    full[core] = mine[:, own_rows]
    for load in loads[3:5]:
        load.wait()
    last_copy.wait()
    parts = []
    for i, weight in enumerate((wo, co)):
        parts.append(matmul(jnp.concatenate([full[0, i], full[1, i]], axis=1), weight[...]))
    result = (hidden.astype(jnp.float32) + parts[0] + parts[1] + mlp_part).astype(jnp.bfloat16)
    outs_refs[0][...] = result
    if not last:
        store_normed(x_ref, result, gain_ref[layer + 1:layer + 2, :])
        run_gather(x_ref, h_ref, refs[29:], pos, core)
        for load in next_loads:
            load.wait()
        self_body(pos, h_ref, w_ref, k_ref, v_ref, q_ref, outs_refs[1], outs_refs[2])
    for one in copies.values():
        one.wait_send()


def finish_layer(layer, last, partial, att, hidden, gain, w1, w3, w2, wo, co, next_weights=(), memory=None):
    f32, bf16 = jnp.float32, jnp.bfloat16
    n_rows, half = att.shape
    rows, width = hidden.shape
    ff = w1.shape[2]
    third = width // 3
    out_shape = [jax.ShapeDtypeStruct(hidden.shape, bf16)]
    if not last:
        out_shape += att_shapes(rows, width)
        out_shape += [jax.ShapeDtypeStruct((1, memory.shape[0], half), bf16),
                      jax.ShapeDtypeStruct((1, half, memory.shape[0]), bf16)]
    return pl.pallas_call(
        functools.partial(finish_kernel, layer, last),
        out_shape=out_shape,
        in_specs=[VMEM_SPEC] * 4 + [HBM_SPEC] * (5 + len(next_weights)) + ([] if last else [VMEM_SPEC]),
        out_specs=[VMEM_SPEC] * len(out_shape),
        scratch_shapes=[pltpu.VMEM((width, ff), bf16), pltpu.VMEM((width, ff), bf16), pltpu.VMEM((ff, width), bf16),
                        pltpu.VMEM((width, width), bf16), pltpu.VMEM((width, width), bf16),
                        pltpu.VMEM((3, 3, 4, PART_ROWS, LANES), f32), pltpu.VMEM((3, 4, PART_ROWS, LANES), f32),
                        pltpu.VMEM((3, 3, PART_ROWS, LANES), f32), pltpu.VMEM((3, PART_ROWS, LANES), f32),
                        pltpu.VMEM((3, 3, PART_ROWS, LANES), f32), pltpu.VMEM((3, LANES, LANES), f32),
                        pltpu.VMEM((2, n_rows, half), bf16), pltpu.VMEM((2, 2, rows, half), bf16),
                        pltpu.VMEM((3, rows, third), bf16),
                        pltpu.SemaphoreType.DMA((5,)), CUT_SEMS, CUT_SEMS,
                        PHASE_SEMS, PHASE_SEMS,
                        pltpu.SemaphoreType.DMA, pltpu.SemaphoreType.DMA]
        + ([] if last else [pltpu.VMEM((width, width), bf16), pltpu.SemaphoreType.DMA((2,))]
           + self_scratch(rows, width) + GATHER_SEMS),
        compiler_params=pltpu.CompilerParams(collective_id=1 + layer, has_side_effects=True,
                                             vmem_limit_bytes=36 * 1024 * 1024),
        name="finish_layer",
    )(partial, att, hidden, gain, *map(in_hbm, (w1, w3, w2, wo, co) + next_weights), *([] if last else [memory]))


def solution(mesh):
    row_spec = P(("dp", "sp"), None)
    full_spec = P()

    def device_step(y_dec, memory, mem_len, norm_gain, self_wq, self_wk, self_wv, self_wo, cross_wq, cross_wk, cross_wv, cross_wo, mlp_gate, mlp_up, mlp_down):
        tq_dev, width = y_dec.shape
        tm_dev = memory.shape[0]
        sp = lax.axis_index("sp")
        chip = sp // 2
        tiles = [jnp.where(spread_start(chip, z, 0) < mem_len[0], 1, 0) for z in PARTS]
        info = jnp.stack([chip, sp % 2, mem_len[0], sum(tiles)]).astype(jnp.int32)
        weights = (self_wk, self_wv, cross_wq, self_wq)
        att, qt, rows = first_layer(y_dec, norm_gain, memory, *weights)
        rows = rows.reshape(3 * tm_dev // 2, width)
        keys, values = memory_kv(info, rows, cross_wk, cross_wv)
        hidden = y_dec
        layers = norm_gain.shape[0]
        for layer in range(layers):
            partial = cross_attention(info, qt, keys, values)
            last = layer == layers - 1
            out = finish_layer(layer, last, partial, att, hidden, norm_gain, mlp_gate, mlp_up, mlp_down, self_wo,
                               cross_wo, *(() if last else (weights + (cross_wk, cross_wv), rows)))
            hidden = out[0]
            if not last:
                att, qt, keys, values = out[1:]
        return hidden

    return jax.shard_map(device_step, mesh=mesh, in_specs=(row_spec, row_spec, P("dp")) + (full_spec,) * 12, out_specs=row_spec, check_vma=False)
```
